32 devices in a mesh: gx: 2 (over x), gy: 16 (over z, y, core).
Axes of the slice: x: 2, y: 2, z: 4, core: 2. Of those that a mesh axis runs over, the one named last changes fastest.
Arguments:
- right_side: float32 [262144], P(('gx', 'gy')), may hold values from -60 to 60
- reaction: float32 [262144], P(('gx', 'gy')), may hold values from 0.5 to 2
- cell_slots: int32 [125, 4096], P(None, ('gx', 'gy')), may hold values from 0 to 12543
- cell_level: int32 [4096], P(('gx', 'gy')), may hold values from 0 to 2
- con_masters: int32 [5, 8192], P(None, ('gx', 'gy')), may hold values from 0 to 12287
- con_rows: int32 [8192], P(('gx', 'gy')), may hold values from 0 to 9
- send_lists: int32 [8, 16384], P(None, ('gx', 'gy')), may hold values from 0 to 8191
Outputs:
- solution: float32 [262144], P(('gx', 'gy'))
- residual: float32 [262144], P(('gx', 'gy'))
The draws below stay inside these ranges and needn't reach their ends.
Inputs may be any that keep to these rules, and one draw needn't show every extreme that they name: `cell_slots`: column block of rank d indexes d's local list: its 8192 owned unknowns, then 512 values from each of ranks d - 1, ..., d - 4, then from d + 1, ..., d + 4, then its 256 constrained values (rank d = 16 gx + gy). `cell_level`: A cell of level l has side 2^(-l). `con_masters`: slots among the same rank's owned and ghost values. `con_rows`: row of the interpolation table: 5 fine nodes on each half of a coarse edge. `send_lists`: row j of rank s lists s's owned unknowns that fill ghost block j of rank s + j + 1 (j < 4) or of rank s - (j - 3); rows without such a rank are unused.
All inputs are finite; a program needn't handle non-finite values.
Results may differ from the reference program's by a relative error of at most 0.0002.
Values sent between devices are 32-bit elements; how exact they have to be, the bound alone decides.
A program may use at most 64 MiB of HBM per device.

```python
import math
import jax
import jax.numpy as jnp
import numpy as np
from jax import lax

NODES = 5
PEERS = 4
ITERS = 3
CELLS_DEV = 128
NOWN = 8192
GHOSTS = 512
NCON = 256
CELLS = 4096
NDOF = 262144
NCON_ALL = 8192
LISTS = 16384
N_GX = 2
N_GY = 16


def draw_right_side(key, part):
    entries = NDOF
    position = jnp.arange(entries, dtype=jnp.float32) / entries
    rising = 1.0 + 2.0 * position
    first_key = jax.random.fold_in(jax.random.fold_in(key, 11), 0)
    normal_part = jnp.clip(jax.random.normal(first_key, (entries,), jnp.float32), -4.0, 4.0)
    return (normal_part * rising).astype(jnp.float32)


def set_ends(drawn, own_key, low, largest):
    extent = drawn.shape
    spot = [jax.random.randint(jax.random.fold_in(own_key, axis), (), 0, extent[axis]) for axis in range(len(extent))]
    drawn = drawn.at[tuple(spot)].set(low)
    longest = extent.index(max(extent))
    spot[longest] = (spot[longest] + 1) % extent[longest]
    return drawn.at[tuple(spot)].set(largest)


def block_levels(stream_key, shape, cuts, smallest, largest):
    def one(dim, shards_of):
        steps = jax.random.uniform(jax.random.fold_in(jax.random.fold_in(stream_key, 6), dim), (shards_of,), jnp.float32, smallest / len(cuts), largest / len(cuts))
        return jnp.repeat(jnp.exp(steps), shape[dim] // shards_of).reshape((-1,) + (1,) * (len(shape) - dim - 1))

    gain = one(*cuts[0])
    for cut in cuts[1:]:
        gain = gain * one(*cut)
    return gain


def setup_inputs(seed: int = 0) -> dict:
    key_list = jax.random.split(jax.random.key(seed), 8)
    return {
        "right_side": draw_right_side(jax.random.fold_in(key_list[7], 71), 0),
        "reaction": jnp.clip(jnp.exp(math.log(2.0) - 1.3862944 * jax.random.uniform(key_list[1], (NDOF,), jnp.float32) ** block_levels(key_list[1], (NDOF,), ((0, 32),), -0.2, 0.2)), 0.5, 2.0),
        "cell_slots": set_ends(jax.random.randint(key_list[2], (NODES ** 3, CELLS), 0, NOWN + 2 * PEERS * GHOSTS + NCON), jax.random.fold_in(key_list[2], 1), 0, (NOWN + 2 * PEERS * GHOSTS + NCON) - 1).astype(jnp.int32),
        "cell_level": set_ends(jax.random.randint(key_list[3], (CELLS,), 0, 3), jax.random.fold_in(key_list[3], 1), 0, 2).astype(jnp.int32),
        "con_masters": set_ends(jax.random.randint(key_list[4], (NODES, NCON_ALL), 0, NOWN + 2 * PEERS * GHOSTS), jax.random.fold_in(key_list[4], 1), 0, (NOWN + 2 * PEERS * GHOSTS) - 1).astype(jnp.int32),
        "con_rows": set_ends(jax.random.randint(key_list[5], (NCON_ALL,), 0, 10), jax.random.fold_in(key_list[5], 1), 0, 9).astype(jnp.int32),
        "send_lists": set_ends(jax.random.randint(key_list[6], (2 * PEERS, LISTS), 0, NOWN), jax.random.fold_in(key_list[6], 1), 0, NOWN - 1).astype(jnp.int32),
    }


def lagrange(node_list, points):
    node_count = len(node_list)
    values = np.ones((len(points), node_count))
    derivs = np.zeros((len(points), node_count))
    for basis_node in range(node_count):
        for other_node in range(node_count):
            if other_node != basis_node:
                values[:, basis_node] = values[:, basis_node] * (points - node_list[other_node]) / (node_list[basis_node] - node_list[other_node])
        for skipped in range(node_count):
            if skipped != basis_node:
                product_term = np.ones(len(points)) / (node_list[basis_node] - node_list[skipped])
                for other_node in range(node_count):
                    if other_node != basis_node and other_node != skipped:
                        product_term = product_term * (points - node_list[other_node]) / (node_list[basis_node] - node_list[other_node])
                derivs[:, basis_node] = derivs[:, basis_node] + product_term
    return (values, derivs)

def tables():
    gll_offset = np.sqrt(3.0 / 7.0)
    lobatto = np.array([0.0, (1.0 - gll_offset) / 2.0, 0.5, (1.0 + gll_offset) / 2.0, 1.0])
    inner_point = np.sqrt(5.0 - 2.0 * np.sqrt(10.0 / 7.0)) / 3.0
    outer_point = np.sqrt(5.0 + 2.0 * np.sqrt(10.0 / 7.0)) / 3.0
    inner_weight = (322.0 + 13.0 * np.sqrt(70.0)) / 900.0
    outer_weight = (322.0 - 13.0 * np.sqrt(70.0)) / 900.0
    points = np.array([-outer_point, -inner_point, 0.0, inner_point, outer_point])
    gauss_weights = np.array([outer_weight, inner_weight, 128.0 / 225.0, inner_weight, outer_weight])
    points = (points + 1.0) / 2.0
    gauss_weights = gauss_weights / 2.0
    shapes, slopes = lagrange(lobatto, points)
    fine_points = np.concatenate([lobatto / 2.0, (1.0 + lobatto) / 2.0])
    interp, unused_slopes = lagrange(lobatto, fine_points)
    quad_weights = np.kron(gauss_weights, np.kron(gauss_weights, gauss_weights))
    grad_x = np.kron(slopes, np.kron(shapes, shapes))
    grad_y = np.kron(shapes, np.kron(slopes, shapes))
    grad_z = np.kron(shapes, np.kron(shapes, slopes))
    stiffness = np.zeros((125, 125))
    for gradient in (grad_x, grad_y, grad_z):
        stiffness = stiffness + gradient.T @ (quad_weights[:, None] * gradient)
    return (jnp.asarray(interp, jnp.float32), jnp.asarray(stiffness, jnp.float32))

def cell_laplace(cell_values, cell_scale, stiffness):
    product = jnp.dot(stiffness, cell_values, precision=lax.Precision.HIGHEST, preferred_element_type=jnp.float32)
    return product * cell_scale[None, :]

def local_apply(own_values, ghosts, slot_map, cell_scale, masters, weights, stiffness):
    local_list = jnp.concatenate([own_values, ghosts.reshape(-1)])
    picked = local_list[masters]
    resolved = lax.optimization_barrier(jnp.sum(weights * picked, axis=0))
    full_list = jnp.concatenate([local_list, resolved])
    cell_values = full_list[slot_map]
    contrib = cell_laplace(cell_values, cell_scale, stiffness)
    summed = jnp.zeros(full_list.shape, jnp.float32).at[slot_map.reshape(-1)].add(contrib.reshape(-1))
    split_at = local_list.shape[0]
    spread = summed[:split_at].at[masters.reshape(-1)].add((weights * summed[split_at:][None, :]).reshape(-1))
    return spread

def reference(right_side, reaction, cell_slots, cell_level, con_masters, con_rows, send_lists):
    interp, stiffness = tables()
    rank_count = N_GX * N_GY
    block_count = 2 * PEERS
    offsets = [neighbour + 1 for neighbour in range(PEERS)] + [-(neighbour + 1) for neighbour in range(PEERS)]
    slot_maps = cell_slots.reshape(125, rank_count, CELLS_DEV).transpose(1, 0, 2)
    scales = jnp.exp2(-cell_level.astype(jnp.float32)).reshape(rank_count, CELLS_DEV)
    master_maps = con_masters.reshape(5, rank_count, NCON).transpose(1, 0, 2)
    selector = (con_rows.reshape(rank_count, NCON)[:, None, :] == jnp.arange(10, dtype=jnp.int32)[None, :, None]).astype(jnp.float32)
    weight_maps = jnp.einsum('tk,rtn->rkn', interp, selector, precision=lax.Precision.HIGHEST)
    list_rows = send_lists.reshape(block_count, rank_count, GHOSTS).transpose(1, 0, 2)
    rank_ids = jnp.arange(rank_count, dtype=jnp.int32)
    reactions = reaction.reshape(rank_count, NOWN)
    source_ids = [rank_ids - offset for offset in offsets]
    inside = [(source >= 0) & (source < rank_count) for source in source_ids]
    owner_ids = [jnp.clip(source, 0, rank_count - 1).astype(jnp.int32) for source in source_ids]

    def one_rank(packed):
        own_values, ghost_values, slot_map, cell_scale, masters, weights = packed
        return local_apply(own_values, ghost_values, slot_map, cell_scale, masters, weights, stiffness)

    def operate(vector):
        field_rows = vector.reshape(rank_count, NOWN)
        ghost_parts = []
        for neighbour in range(block_count):
            fetched = field_rows[owner_ids[neighbour][:, None], list_rows[owner_ids[neighbour], neighbour]]
            ghost_parts.append(jnp.where(inside[neighbour][:, None], fetched, 0.0))
        ghosts = jnp.stack(ghost_parts, axis=1)
        spread = lax.map(one_rank, (field_rows, ghosts, slot_maps, scales, master_maps, weight_maps))
        result = (spread[:, :NOWN] + reactions * field_rows).reshape(-1)
        returned = spread[:, NOWN:].reshape(rank_count, block_count, GHOSTS)
        for neighbour in range(block_count):
            target = owner_ids[neighbour][:, None] * NOWN + list_rows[owner_ids[neighbour], neighbour]
            addend = jnp.where(inside[neighbour][:, None], returned[:, neighbour], 0.0)
            result = result.at[target.reshape(-1)].add(addend.reshape(-1))
        return result
    solution = jnp.zeros_like(right_side)
    residual = right_side
    direction = right_side
    norm_now = jnp.sum(residual * residual)
    for iteration in range(ITERS):
        applied = operate(direction)
        step_size = norm_now / jnp.sum(direction * applied)
        solution = solution + step_size * direction
        residual = residual - step_size * applied
        norm_next = jnp.sum(residual * residual)
        direction = residual + norm_next / norm_now * direction
        norm_now = norm_next
    return (solution, residual)
```

```python
import functools

import jax
import jax.numpy as jnp
import numpy as np
from jax import lax
from jax.experimental import pallas as pl
from jax.experimental.pallas import tpu as pltpu
from jax.sharding import PartitionSpec as P

ITERS = 3
LANES = 128
SUMS = 4
ROUNDS = 2
UNROLL = 9
MESH = pl.DeviceIdType.MESH


def lagrange(node_list, points):
    node_count = len(node_list)
    values = np.ones((len(points), node_count))
    derivs = np.zeros((len(points), node_count))
    for basis_node in range(node_count):
        for other_node in range(node_count):
            if other_node != basis_node:
                values[:, basis_node] = (
                    values[:, basis_node]
                    * (points - node_list[other_node])
                    / (node_list[basis_node] - node_list[other_node])
                )
        for skipped in range(node_count):
            if skipped != basis_node:
                product_term = np.ones(len(points)) / (node_list[basis_node] - node_list[skipped])
                for other_node in range(node_count):
                    if other_node != basis_node and other_node != skipped:
                        product_term = (
                            product_term
                            * (points - node_list[other_node])
                            / (node_list[basis_node] - node_list[other_node])
                        )
                derivs[:, basis_node] = derivs[:, basis_node] + product_term
    return (values, derivs)


def tables():
    gll_offset = np.sqrt(3.0 / 7.0)
    lobatto = np.array([0.0, (1.0 - gll_offset) / 2.0, 0.5, (1.0 + gll_offset) / 2.0, 1.0])
    inner_point = np.sqrt(5.0 - 2.0 * np.sqrt(10.0 / 7.0)) / 3.0
    outer_point = np.sqrt(5.0 + 2.0 * np.sqrt(10.0 / 7.0)) / 3.0
    inner_weight = (322.0 + 13.0 * np.sqrt(70.0)) / 900.0
    outer_weight = (322.0 - 13.0 * np.sqrt(70.0)) / 900.0
    points = np.array([-outer_point, -inner_point, 0.0, inner_point, outer_point])
    gauss_weights = np.array(
        [outer_weight, inner_weight, 128.0 / 225.0, inner_weight, outer_weight]
    )
    points = (points + 1.0) / 2.0
    gauss_weights = gauss_weights / 2.0
    shapes, slopes = lagrange(lobatto, points)
    fine_points = np.concatenate([lobatto / 2.0, (1.0 + lobatto) / 2.0])
    interp, unused_slopes = lagrange(lobatto, fine_points)
    quad_weights = np.kron(gauss_weights, np.kron(gauss_weights, gauss_weights))
    grad_x = np.kron(slopes, np.kron(shapes, shapes))
    grad_y = np.kron(shapes, np.kron(slopes, shapes))
    grad_z = np.kron(shapes, np.kron(shapes, slopes))
    stiffness = np.zeros((125, 125))
    for gradient in (grad_x, grad_y, grad_z):
        stiffness = stiffness + gradient.T @ (quad_weights[:, None] * gradient)
    return (interp.astype(np.float32), stiffness.astype(np.float32))


def round_up(value, step):
    return -(-value // step) * step


def split(value):
    high = value.astype(jnp.bfloat16)
    low = (value - high.astype(jnp.float32)).astype(jnp.bfloat16)
    return high, low


def kernel(
    shape,
    interp,
    *refs,
):
    inputs, refs = refs[:8], refs[8:]
    answer_ref, ahead_ref, residual_ref, applied_ref, step_ref = refs[:5]
    staged, refs = refs[5:13], refs[13:]
    right_ref, reaction_ref, cells_ref, level_ref, masters_ref, rows_ref, lists_ref, stiff_ref = staged
    (
    load_sem,
    own_values,
    own_table,
    onehot,
    lane_of,
    row_of,
    weights,
    cell_buf,
    own_acc,
    far_acc,
    con_acc,
    out_src,
    out_dst,
    back_src,
    back_dst,
    part,
    first_buf,
    mid_part,
    second_buf,
    out_send,
    out_recv,
    back_send,
    back_recv,
    first_send,
    first_recv,
    second_send,
    second_recv,
    ) = refs
    loads = [
        pltpu.make_async_copy(source, target, load_sem.at[i])
        for i, (source, target) in enumerate(zip(inputs, staged))
    ]
    order = [0, 6, 2, 4, 5, 3, 1, 7]
    for i in order:
        loads[i].start()
    nx, ny = shape
    count = nx * ny
    inner = lax.axis_index("gy")
    me = lax.axis_index("gx") * ny + inner
    upper = lax.div(2 * inner, ny)

    def place(rank):
        return (lax.div(rank, ny), lax.rem(rank, ny))

    blocks, listed = lists_ref.shape
    half = blocks // 2
    own_rows = right_ref.shape[0]
    block_rows = listed // LANES
    ghost_rows = blocks * block_rows
    side_rows = half * block_rows
    con_rows = rows_ref.shape[0]
    con_pad = round_up(con_rows, 8)
    far_rows = ghost_rows + con_pad
    nodes = masters_ref.shape[0]
    points = cells_ref.shape[0]
    cell_rows = round_up(points, 8)
    cell_groups = cell_rows // 8
    list_groups = ghost_rows // 8
    side_groups = list_groups // 2
    per_group = 8 // block_rows
    con_base = cell_groups
    work_groups = cell_groups + con_rows
    list_base = work_groups
    near, far = phases(count)
    near_id, far_id = lax.rem(me, near), lax.div(me, near)
    sent_first = 1 - upper

    def offset(side, k):
        return (k + 1) * (1 - 2 * side)

    def near_peer(step):
        return far_id * near + lax.rem(near_id + step, near)

    def far_peer(step):
        return lax.rem(far_id + step, far) * near + near_id

    def ring_peer(distance):
        return lax.rem(me + distance + count, count)

    barrier = pltpu.get_barrier_semaphore()
    peers = [ring_peer(offset(side, k)) for side in range(2) for k in range(half)]
    peers += [near_peer(step) for step in range(1, near)]
    peers += [far_peer(step) for step in range(1, far)]
    for peer in peers:
        pl.semaphore_signal(barrier, inc=1, device_id=place(peer), device_id_type=MESH)

    def put(at, slots, shown):
        size = slots.shape[0]
        for copy in range(2 * ITERS):
            lane_of[copy, at : at + size, :] = lax.rem(slots, LANES)
        row_of[at : at + size, :] = jnp.where(shown, lax.div(slots, LANES), -1)

    def held(slots):
        rows = lax.div(slots, LANES) - own_rows
        shown = jnp.full(slots.shape, True)
        for side in range(2):
            for k in range(half):
                other = me - offset(side, k)
                low = (side * half + k) * block_rows
                outside = jnp.logical_or(other < 0, other >= count)
                hidden = jnp.logical_and(rows >= low, rows < low + block_rows)
                shown = jnp.logical_and(shown, jnp.logical_not(jnp.logical_and(hidden, outside)))
        return shown

    lane_iota = lax.broadcasted_iota(jnp.int32, (LANES, LANES), 0)

    def build(g, carry):
        lanes = lane_of[0, pl.ds(pl.multiple_of(g * 8, 8), 8), :]
        for i in range(8):
            hit = jnp.where(lanes[i : i + 1, :] == lane_iota, 1.0, 0.0)
            onehot[g, :, i * LANES : (i + 1) * LANES] = hit.astype(jnp.bfloat16)
        return carry

    iota8 = lax.broadcasted_iota(jnp.int32, (8, LANES), 0)

    once = 1 + lax.div(inner, ny)

    def apart(work):
        def body(i, carry):
            work()
            return carry

        lax.fori_loop(0, once, body, 0)

    def group(g):
        return pl.ds(pl.multiple_of(g * 8, 8), 8)

    def gather(g, table):
        depth = table.shape[0] // 2
        spread = jnp.dot(table[...], onehot[g], preferred_element_type=jnp.float32)
        rows = row_of[group(g), :]
        found = []
        for i in range(8):
            wanted = jnp.broadcast_to(rows[i : i + 1, :], (8, LANES)) - iota8
            high = jnp.zeros((8, LANES), jnp.float32)
            low = high
            for k in range(depth // 8):
                hit = wanted == 8 * k
                at, cols = 8 * k, slice(i * LANES, (i + 1) * LANES)
                high = jnp.where(hit, spread[at : at + 8, cols], high)
                low = jnp.where(hit, spread[depth + at : depth + at + 8, cols], low)
            found.append(jnp.sum(high + low, axis=0, keepdims=True))
        return jnp.concatenate(found, axis=0)

    def pick(lanes, rows, lines, found):
        for k, line in enumerate(lines):
            moved = jnp.take_along_axis(
                jnp.broadcast_to(line, (8, LANES)), lanes, axis=1, mode="promise_in_bounds"
            )
            found = jnp.where(rows == k, moved, found)
        return found

    def parts_of(values):
        high = values.astype(jnp.bfloat16).astype(jnp.float32)
        return high, values - high

    def against(placed, g):
        return lax.dot_general(
            placed, onehot[g], (((1,), (1,)), ((), ())), preferred_element_type=jnp.float32
        )

    def scatter(g, values, base, depth):
        rows = row_of[group(g), :] - base
        high, low = parts_of(values)
        row_iota = lax.broadcasted_iota(jnp.int32, (depth, LANES), 0)
        columns = []
        for i in range(8):
            hit = rows[i : i + 1, :] == row_iota
            upper_part = jnp.where(hit, high[i : i + 1, :], 0.0).astype(jnp.bfloat16)
            lower_part = jnp.where(hit, low[i : i + 1, :], 0.0).astype(jnp.bfloat16)
            columns.append(jnp.concatenate([upper_part, lower_part], axis=0))
        return against(jnp.concatenate(columns, axis=1), g)

    def scatter_far(g, values):
        rows = row_of[group(g), :] - own_rows
        high, low = parts_of(values)
        row_iota = lax.broadcasted_iota(jnp.int32, (ghost_rows, LANES), 0)
        con_iota = lax.broadcasted_iota(jnp.int32, (2 * con_pad, LANES), 0)
        con_row = ghost_rows + lax.rem(con_iota, con_pad)
        columns = []
        for i in range(8):
            one = rows[i : i + 1, :]
            hit = one == row_iota
            con_hit = one == con_row
            top, bottom = high[i : i + 1, :], low[i : i + 1, :]
            both = jnp.where(con_iota < con_pad, top, bottom)
            columns.append(
                jnp.concatenate(
                    [
                        jnp.where(hit, top, 0.0).astype(jnp.bfloat16),
                        jnp.where(hit, bottom, 0.0).astype(jnp.bfloat16),
                        jnp.where(con_hit, both, 0.0).astype(jnp.bfloat16),
                    ],
                    axis=0,
                )
            )
        placed = jnp.concatenate(columns, axis=1)
        return lax.dot_general(
            onehot[g], placed, (((1,), (1,)), ((), ())), preferred_element_type=jnp.float32
        )

    def folded(both):
        depth = both.shape[0] // 2
        return both[0:depth] + both[depth : 2 * depth]

    def store(table, value):
        high, low = split(value)
        size = value.shape[0]
        table[0:size, :] = high
        table[size : 2 * size, :] = low

    def out_copy(turn, side, k):
        j = side * half + k
        return pltpu.make_async_remote_copy(
            src_ref=out_src.at[turn, j],
            dst_ref=out_dst.at[turn, j],
            send_sem=out_send.at[side],
            recv_sem=out_recv.at[side],
            device_id=place(ring_peer(offset(side, k))),
            device_id_type=MESH,
        )

    def back_copy(turn, side, k):
        j = side * half + k
        return pltpu.make_async_remote_copy(
            src_ref=back_src.at[turn, j],
            dst_ref=back_dst.at[turn, j],
            send_sem=back_send.at[side],
            recv_sem=back_recv.at[side],
            device_id=place(ring_peer(-offset(side, k))),
            device_id_type=MESH,
        )

    def near_copy(turn, step):
        return pltpu.make_async_remote_copy(
            src_ref=part.at[turn],
            dst_ref=first_buf.at[turn, near_id],
            send_sem=first_send.at[turn],
            recv_sem=first_recv.at[turn],
            device_id=place(near_peer(step)),
            device_id_type=MESH,
        )

    def far_copy(turn, step):
        return pltpu.make_async_remote_copy(
            src_ref=mid_part.at[turn],
            dst_ref=second_buf.at[turn, far_id],
            send_sem=second_send.at[turn],
            recv_sem=second_recv.at[turn],
            device_id=place(far_peer(step)),
            device_id_type=MESH,
        )

    out_ends = (out_src, out_dst, out_send, out_recv)
    back_ends = (back_src, back_dst, back_send, back_recv)

    def lists_of(turn, side):
        found = []
        lines = [own_values[r : r + 1, :] for r in range(own_rows)]
        for q in range(side_groups):
            at = group(list_base + side * side_groups + q)
            zero = jnp.zeros((8, LANES), jnp.float32)
            found.append(pick(lane_of[2 * turn, at, :], row_of[at, :], lines, zero))
        return found

    def send_lists(turn, side, found):
        for q in range(side_groups):
            for r in range(per_group):
                j = side * half + q * per_group + r
                out_src[turn, j] = found[q][r * block_rows : (r + 1) * block_rows]

    def arrived(turn, side, mixed):
        source = turn
        if mixed is not None:
            source = ITERS
            for k in range(half):
                j = side * half + k
                out_dst[source, j] = mixed(*[out_dst[t, j] for t in range(turn + 1)])
        return [
            out_dst[source, side * half + k, r : r + 1, :] for k in range(half) for r in range(block_rows)
        ]

    def settle(ref, sem):
        pltpu.make_async_copy(ref, ref, sem).wait()

    def finish(ends, turn, side):
        source, target, send_sem, recv_sem = ends
        some = pl.ds(side * half, half)
        settle(source.at[turn, some], send_sem.at[side])
        settle(target.at[turn, some], recv_sem.at[side])

    def begin_apply(turn, vector):
        own_values[...] = vector
        for side in (sent_first, upper):
            send_lists(turn, side, lists_of(turn, side))
            if turn == 0 and side is sent_first:
                pl.semaphore_wait(barrier, len(peers))
            for k in range(half):
                out_copy(turn, side, k).start()

    def apply(turn, vector, mixed, begin, middle):
        store(own_table, vector)

        def take_own(g, carry):
            cell_buf[group(g), :] = gather(g, own_table)
            return carry

        lax.fori_loop(0, work_groups, take_own, 0, unroll=UNROLL)

        finish(out_ends, turn, sent_first)
        early, late = sent_first, upper
        lines = arrived(turn, early, mixed)
        base = own_rows + early * side_rows
        for g in range(work_groups):
            at = slice(8 * g, 8 * g + 8)
            cell_buf[at, :] = pick(lane_of[2 * turn, at, :], row_of[at, :] - base, lines, cell_buf[at, :])

        finish(out_ends, turn, late)
        lines = arrived(turn, late, mixed)
        base = own_rows + late * side_rows
        resolved = []
        for h in range(con_rows):
            at, to = slice(8 * (con_base + h), 8 * (con_base + h) + 8), slice(8 * h, 8 * h + 8)
            found = pick(lane_of[2 * turn + 1, at, :], row_of[at, :] - base, lines, cell_buf[at, :])
            resolved.append(jnp.sum(weights[to, :] * found, axis=0, keepdims=True))
        found = []
        for g in range(cell_groups):
            at = slice(8 * g, 8 * g + 8)
            found.append(pick(lane_of[2 * turn + 1, at, :], row_of[at, :] - base, lines, cell_buf[at, :]))
        for g in range(cell_groups):
            at = slice(8 * g, 8 * g + 8)
            rows = row_of[at, :] - (own_rows + ghost_rows)
            found[g] = pick(lane_of[2 * turn + 1, at, :], rows, resolved, found[g])
        nodal = jnp.concatenate(found, axis=0)
        contrib = scale * jnp.dot(
            stiff_ref[...],
            nodal,
            precision=lax.Precision.HIGHEST,
            preferred_element_type=jnp.float32,
        )
        cell_buf[0:cell_rows, :] = contrib
        weighted = reaction_ref[...] * vector
        energy = jnp.sum(nodal * contrib, axis=0, keepdims=True)
        energy = energy + jnp.sum(weighted * vector, axis=0, keepdims=True)
        begin(energy)

        far_acc[...] = jnp.zeros_like(far_acc)

        def give_far(g, carry):
            far_acc[...] += scatter_far(g, cell_buf[group(g), :])
            return carry

        lax.fori_loop(0, cell_groups, give_far, 0, unroll=8)
        total = jnp.transpose(far_acc[...])
        spread = total[0:ghost_rows] + total[ghost_rows : 2 * ghost_rows]
        summed = folded(total[2 * ghost_rows : 2 * far_rows])
        for h in range(con_rows):
            shares = weights[8 * h : 8 * h + 8, :] * summed[h : h + 1]
            cell_buf[8 * (con_base + h) : 8 * (con_base + h) + 8, :] = shares

        def give_con():
            total = jnp.zeros((2 * ghost_rows, LANES), jnp.float32)
            for h in range(con_rows):
                values = cell_buf[8 * (con_base + h) : 8 * (con_base + h) + 8, :]
                total = total + scatter(con_base + h, values, own_rows, ghost_rows)
            con_acc[...] = total

        apart(give_con)
        spread = spread + folded(con_acc[...])
        for j in range(blocks):
            back_src[turn, j] = spread[j * block_rows : (j + 1) * block_rows]
        for side in (late, early):
            for k in range(half):
                back_copy(turn, side, k).start()
        middle()
        own_acc[...] = jnp.zeros_like(own_acc)

        def give_own(g, carry):
            own_acc[...] += scatter(g, cell_buf[group(g), :], 0, own_rows)
            return carry

        lax.fori_loop(0, work_groups, give_own, 0, unroll=UNROLL)
        for side in (late, early):
            finish(back_ends, turn, side)

            def give_list(side=side):
                both = own_acc[...]
                for q in range(side_groups):
                    j = side * half + q * per_group
                    values = jnp.concatenate([back_dst[turn, j + r] for r in range(per_group)], axis=0)
                    both = both + scatter(list_base + side * side_groups + q, values, 0, own_rows)
                own_acc[...] = both

            apart(give_list)
        both = own_acc[...]
        return folded(both) + weighted

    def dot(one, two):
        return jnp.sum(one * two, axis=0, keepdims=True)

    lane = lax.broadcasted_iota(jnp.int32, (1, LANES), 1)
    width = LANES // SUMS

    def sums_start(turn, parts):
        total = jnp.sum(jnp.concatenate(parts, axis=0), axis=1, keepdims=True)
        mine = jnp.zeros((1, LANES), jnp.float32)
        for k in range(len(parts)):
            mine = jnp.where(lax.div(lane, width) == k, total[k : k + 1], mine)
        part[turn] = mine
        first_buf[turn, near_id] = mine

    def sums_send(turn):
        for step in range(1, near):
            near_copy(turn, step).start()

    def near_total(turn):
        others = pl.ds(0, near - 1)
        settle(first_buf.at[turn, others], first_send.at[turn])
        settle(first_buf.at[turn, others], first_recv.at[turn])
        mine = first_buf[turn, 0]
        for k in range(1, near):
            mine = mine + first_buf[turn, k]
        return mine

    def sums_middle(turn):
        sums_send(turn)
        if far == 1:
            return
        mine = near_total(turn)
        mid_part[turn] = mine
        second_buf[turn, far_id] = mine
        for step in range(1, far):
            far_copy(turn, step).start()

    def sums_end(turn):
        if far == 1:
            total = near_total(turn)
        else:
            others = pl.ds(0, far - 1)
            settle(second_buf.at[turn, others], second_send.at[turn])
            settle(second_buf.at[turn, others], second_recv.at[turn])
            total = second_buf[turn, 0]
            for k in range(1, far):
                total = total + second_buf[turn, k]
        return [total[:, k * width : k * width + 1] for k in range(SUMS)]

    loads[0].wait()
    loads[6].wait()
    for side in range(2):
        for k in range(half):
            j = side * half + k
            other = me + offset(side, k)
            inside = jnp.logical_and(other >= 0, other < count)
            for q in range(block_rows):
                at = list_base * 8 + j * block_rows + q
                put(at, lists_ref[j : j + 1, q * LANES : (q + 1) * LANES], inside)
    start = right_ref[...]
    begin_apply(0, start)
    for i in order[2:]:
        loads[i].wait()
    for copy in range(2 * ITERS):
        lane_of[copy, points:cell_rows, :] = jnp.zeros((cell_rows - points, LANES), jnp.int32)
    row_of[points:cell_rows, :] = jnp.full((cell_rows - points, LANES), -1, jnp.int32)
    slots = cells_ref[...]
    put(0, slots, held(slots))
    weights[...] = jnp.zeros_like(weights)
    for h in range(con_rows):
        at = (con_base + h) * 8
        for copy in range(2 * ITERS):
            lane_of[copy, at : at + 8, :] = jnp.zeros((8, LANES), jnp.int32)
        row_of[at : at + 8, :] = jnp.full((8, LANES), -1, jnp.int32)
        slots = masters_ref[:, h * LANES : (h + 1) * LANES]
        put(at, slots, held(slots))
        chosen = rows_ref[h : h + 1, :]
        for k in range(nodes):
            weight = jnp.zeros((1, LANES), jnp.float32)
            for t in range(interp.shape[0]):
                weight = jnp.where(chosen == t, float(interp[t, k]), weight)
            weights[h * 8 + k : h * 8 + k + 1, :] = weight
    lax.fori_loop(0, onehot.shape[0], build, 0)
    scale = jnp.exp2(-level_ref[...].astype(jnp.float32))

    first = apply(0, start, None, lambda energy: None, lambda: None)
    begin_apply(1, first)
    known = [dot(start, start), dot(start, first), dot(first, first)]
    second = apply(
        1,
        first,
        None,
        lambda energy: sums_start(0, known + [energy]),
        lambda: sums_middle(0),
    )
    begin_apply(2, second)
    m0, m1, m2, m3 = sums_end(0)
    step0 = m0 / m1
    norm1 = m0 - 2.0 * step0 * m1 + step0 * step0 * m2
    product1 = m1 - 2.0 * step0 * m2 + step0 * step0 * m3
    ratio1 = norm1 / m0
    step1 = norm1 / (product1 - ratio1 * norm1 / step0)

    def next_residual(zeroth, once, twice):
        before = zeroth - step0 * once
        along = once - step0 * twice + ratio1 * once
        return before, along, before - step1 * along

    before, applied_dir, residual = next_residual(start, first, second)
    direction = before + ratio1 * start
    answer = step0 * start + step1 * direction
    square = dot(residual, residual)
    applied = apply(
        2,
        residual,
        lambda *held: next_residual(*held)[2],
        lambda energy: sums_start(1, [square, energy]),
        lambda: sums_middle(1),
    )
    norm2, product2, unused_a, unused_b = sums_end(1)
    ratio2 = norm2 / norm1
    step2 = norm2 / (product2 - ratio2 * norm2 / step1)
    answer_ref[...] = answer
    ahead_ref[...] = residual + ratio2 * direction
    residual_ref[...] = residual
    applied_ref[...] = applied + ratio2 * applied_dir
    step_ref[...] = jnp.broadcast_to(step2, step_ref.shape)


def phases(count):
    if count <= 64:
        return count, 1
    near = 1
    while near * near < count:
        near *= 2
    return near, count // near


def on_device(shape, right_side, reaction, cell_slots, cell_level, con_masters, con_rows, send_lists):
    interp, stiffness = tables()
    own = right_side.shape[0]
    own_rows = own // LANES
    blocks, listed = send_lists.shape
    block_rows = listed // LANES
    con_tiles = con_rows.shape[0] // LANES
    points = cell_slots.shape[0]
    cell_rows = round_up(points, 8)
    far_rows = blocks * block_rows + round_up(con_tiles, 8)
    groups = cell_rows // 8 + blocks * block_rows // 8 + con_tiles
    padded = np.zeros((cell_rows, cell_rows), np.float32)
    padded[:points, :points] = stiffness
    count = shape[0] * shape[1]
    near, far = phases(count)
    operands = [
        right_side.reshape(own_rows, LANES),
        reaction.reshape(own_rows, LANES),
        cell_slots,
        cell_level.reshape(1, -1),
        con_masters,
        con_rows.reshape(con_tiles, LANES),
        send_lists,
        jnp.asarray(padded),
    ]
    exchange = pltpu.VMEM((ITERS, blocks, block_rows, LANES), jnp.float32)
    landing = pltpu.VMEM((ITERS + 1, blocks, block_rows, LANES), jnp.float32)
    tile = jax.ShapeDtypeStruct((own_rows, LANES), jnp.float32)
    line = jax.ShapeDtypeStruct((1, LANES), jnp.float32)
    answer, ahead, residual, applied, step = pl.pallas_call(
        functools.partial(kernel, shape, interp),
        out_shape=(tile, tile, tile, tile, line),
        in_specs=[pl.BlockSpec(memory_space=pl.ANY)] * 8,
        out_specs=(pl.BlockSpec(memory_space=pltpu.VMEM),) * 5,
        scratch_shapes=[
            *[pltpu.VMEM(value.shape, value.dtype) for value in operands],
            pltpu.SemaphoreType.DMA((len(operands),)),
            pltpu.VMEM((own_rows, LANES), jnp.float32),
            pltpu.VMEM((2 * own_rows, LANES), jnp.bfloat16),
            pltpu.VMEM((groups, LANES, 8 * LANES), jnp.bfloat16),
            pltpu.VMEM((2 * ITERS, groups * 8, LANES), jnp.int32),
            pltpu.VMEM((groups * 8, LANES), jnp.int32),
            pltpu.VMEM((con_tiles * 8, LANES), jnp.float32),
            pltpu.VMEM((cell_rows + 8 * con_tiles, LANES), jnp.float32),
            pltpu.VMEM((2 * own_rows, LANES), jnp.float32),
            pltpu.VMEM((LANES, 2 * far_rows), jnp.float32),
            pltpu.VMEM((2 * blocks * block_rows, LANES), jnp.float32),
            exchange,
            landing,
            exchange,
            exchange,
            pltpu.VMEM((ROUNDS, 1, LANES), jnp.float32),
            pltpu.VMEM((ROUNDS, near, 1, LANES), jnp.float32),
            pltpu.VMEM((ROUNDS, 1, LANES), jnp.float32),
            pltpu.VMEM((ROUNDS, far, 1, LANES), jnp.float32),
            pltpu.SemaphoreType.DMA((2,)),
            pltpu.SemaphoreType.DMA((2,)),
            pltpu.SemaphoreType.DMA((2,)),
            pltpu.SemaphoreType.DMA((2,)),
            pltpu.SemaphoreType.DMA((ROUNDS,)),
            pltpu.SemaphoreType.DMA((ROUNDS,)),
            pltpu.SemaphoreType.DMA((ROUNDS,)),
            pltpu.SemaphoreType.DMA((ROUNDS,)),
        ],
        compiler_params=pltpu.CompilerParams(
            collective_id=0, has_side_effects=True, vmem_limit_bytes=60 * 1024 * 1024
        ),
    )(*operands)
    scale = step[0, 0]
    return (
        (answer + scale * ahead).reshape(own),
        (residual - scale * applied).reshape(own),
    )


def solution(mesh):
    placed = (
        P(("gx", "gy")),
        P(("gx", "gy")),
        P(None, ("gx", "gy")),
        P(("gx", "gy")),
        P(None, ("gx", "gy")),
        P(("gx", "gy")),
        P(None, ("gx", "gy")),
    )
    return jax.shard_map(
        functools.partial(on_device, (mesh.shape["gx"], mesh.shape["gy"])),
        mesh=mesh,
        in_specs=placed,
        out_specs=(P(("gx", "gy")), P(("gx", "gy"))),
        check_vma=False,
    )
```

```python
import functools

import jax
import jax.numpy as jnp
import numpy as np
from jax import lax
from jax.experimental import pallas as pl
from jax.experimental.pallas import tpu as pltpu
from jax.sharding import PartitionSpec as P

ITERS = 3
LANES = 128
SUMS = 4
ROUNDS = 2
UNROLL = 9
MESH = pl.DeviceIdType.MESH


def lagrange(node_list, points):
    node_count = len(node_list)
    values = np.ones((len(points), node_count))
    derivs = np.zeros((len(points), node_count))
    for basis_node in range(node_count):
        for other_node in range(node_count):
            if other_node != basis_node:
                values[:, basis_node] = (
                    values[:, basis_node]
                    * (points - node_list[other_node])
                    / (node_list[basis_node] - node_list[other_node])
                )
        for skipped in range(node_count):
            if skipped != basis_node:
                product_term = np.ones(len(points)) / (node_list[basis_node] - node_list[skipped])
                for other_node in range(node_count):
                    if other_node != basis_node and other_node != skipped:
                        product_term = (
                            product_term
                            * (points - node_list[other_node])
                            / (node_list[basis_node] - node_list[other_node])
                        )
                derivs[:, basis_node] = derivs[:, basis_node] + product_term
    return (values, derivs)


def tables():
    gll_offset = np.sqrt(3.0 / 7.0)
    lobatto = np.array([0.0, (1.0 - gll_offset) / 2.0, 0.5, (1.0 + gll_offset) / 2.0, 1.0])
    inner_point = np.sqrt(5.0 - 2.0 * np.sqrt(10.0 / 7.0)) / 3.0
    outer_point = np.sqrt(5.0 + 2.0 * np.sqrt(10.0 / 7.0)) / 3.0
    inner_weight = (322.0 + 13.0 * np.sqrt(70.0)) / 900.0
    outer_weight = (322.0 - 13.0 * np.sqrt(70.0)) / 900.0
    points = np.array([-outer_point, -inner_point, 0.0, inner_point, outer_point])
    gauss_weights = np.array(
        [outer_weight, inner_weight, 128.0 / 225.0, inner_weight, outer_weight]
    )
    points = (points + 1.0) / 2.0
    gauss_weights = gauss_weights / 2.0
    shapes, slopes = lagrange(lobatto, points)
    fine_points = np.concatenate([lobatto / 2.0, (1.0 + lobatto) / 2.0])
    interp, unused_slopes = lagrange(lobatto, fine_points)
    quad_weights = np.kron(gauss_weights, np.kron(gauss_weights, gauss_weights))
    grad_x = np.kron(slopes, np.kron(shapes, shapes))
    grad_y = np.kron(shapes, np.kron(slopes, shapes))
    grad_z = np.kron(shapes, np.kron(shapes, slopes))
    stiffness = np.zeros((125, 125))
    for gradient in (grad_x, grad_y, grad_z):
        stiffness = stiffness + gradient.T @ (quad_weights[:, None] * gradient)
    return (interp.astype(np.float32), stiffness.astype(np.float32))


def round_up(value, step):
    return -(-value // step) * step


def split(value):
    high = value.astype(jnp.bfloat16)
    low = (value - high.astype(jnp.float32)).astype(jnp.bfloat16)
    return high, low


def kernel(
    shape,
    interp,
    *refs,
):
    inputs, refs = refs[:8], refs[8:]
    answer_ref, ahead_ref, residual_ref, applied_ref, step_ref = refs[:5]
    staged, refs = refs[5:13], refs[13:]
    right_ref, reaction_ref, cells_ref, level_ref, masters_ref, rows_ref, lists_ref, stiff_ref = staged
    (
    load_sem,
    own_values,
    own_table,
    onehot,
    lane_of,
    row_of,
    weights,
    cell_buf,
    own_acc,
    far_acc,
    con_acc,
    out_src,
    out_dst,
    back_src,
    back_dst,
    part,
    first_buf,
    mid_part,
    second_buf,
    out_send,
    out_recv,
    back_send,
    back_recv,
    first_send,
    first_recv,
    second_send,
    second_recv,
    ) = refs
    loads = [
        pltpu.make_async_copy(source, target, load_sem.at[i])
        for i, (source, target) in enumerate(zip(inputs, staged))
    ]
    order = [0, 6, 2, 4, 5, 3, 1, 7]
    for i in order:
        loads[i].start()
    nx, ny = shape
    count = nx * ny
    inner = lax.axis_index("gy")
    me = lax.axis_index("gx") * ny + inner
    upper = lax.div(2 * inner, ny)

    def place(rank):
        return (lax.div(rank, ny), lax.rem(rank, ny))

    blocks, listed = lists_ref.shape
    half = blocks // 2
    own_rows = right_ref.shape[0]
    block_rows = listed // LANES
    ghost_rows = blocks * block_rows
    side_rows = half * block_rows
    con_rows = rows_ref.shape[0]
    con_pad = round_up(con_rows, 8)
    far_rows = ghost_rows + con_pad
    nodes = masters_ref.shape[0]
    points = cells_ref.shape[0]
    cell_rows = round_up(points, 8)
    cell_groups = cell_rows // 8
    list_groups = ghost_rows // 8
    side_groups = list_groups // 2
    per_group = 8 // block_rows
    con_base = cell_groups
    work_groups = cell_groups + con_rows
    list_base = work_groups
    near, far = phases(count)
    near_id, far_id = lax.rem(me, near), lax.div(me, near)
    sent_first = 1 - upper
    slow = min(1, half - 1)
    slow_group = slow // per_group
    group_order = [slow_group] + [q for q in range(side_groups) if q != slow_group]
    block_order = [slow] + [k for k in range(half) if k != slow]

    def offset(side, k):
        return (k + 1) * (1 - 2 * side)

    def near_peer(step):
        return far_id * near + lax.rem(near_id + step, near)

    def far_peer(step):
        return lax.rem(far_id + step, far) * near + near_id

    def ring_peer(distance):
        return lax.rem(me + distance + count, count)

    barrier = pltpu.get_barrier_semaphore()
    peers = [ring_peer(offset(side, k)) for side in range(2) for k in range(half)]
    peers += [near_peer(step) for step in range(1, near)]
    peers += [far_peer(step) for step in range(1, far)]
    for peer in peers:
        pl.semaphore_signal(barrier, inc=1, device_id=place(peer), device_id_type=MESH)

    def put(at, slots, shown):
        size = slots.shape[0]
        for copy in range(2 * ITERS):
            lane_of[copy, at : at + size, :] = lax.rem(slots, LANES)
        row_of[at : at + size, :] = jnp.where(shown, lax.div(slots, LANES), -1)

    def held(slots):
        rows = lax.div(slots, LANES) - own_rows
        shown = jnp.full(slots.shape, True)
        for side in range(2):
            for k in range(half):
                other = me - offset(side, k)
                low = (side * half + k) * block_rows
                outside = jnp.logical_or(other < 0, other >= count)
                hidden = jnp.logical_and(rows >= low, rows < low + block_rows)
                shown = jnp.logical_and(shown, jnp.logical_not(jnp.logical_and(hidden, outside)))
        return shown

    lane_iota = lax.broadcasted_iota(jnp.int32, (LANES, LANES), 0)

    def build(g, carry):
        lanes = lane_of[0, pl.ds(pl.multiple_of(g * 8, 8), 8), :]
        for i in range(8):
            hit = jnp.where(lanes[i : i + 1, :] == lane_iota, 1.0, 0.0)
            onehot[g, :, i * LANES : (i + 1) * LANES] = hit.astype(jnp.bfloat16)
        return carry

    iota8 = lax.broadcasted_iota(jnp.int32, (8, LANES), 0)

    once = 1 + lax.div(inner, ny)

    def apart(work):
        def body(i, carry):
            work()
            return carry

        lax.fori_loop(0, once, body, 0)

    def group(g):
        return pl.ds(pl.multiple_of(g * 8, 8), 8)

    def gather(g, table):
        depth = table.shape[0] // 2
        spread = jnp.dot(table[...], onehot[g], preferred_element_type=jnp.float32)
        rows = row_of[group(g), :]
        found = []
        for i in range(8):
            wanted = jnp.broadcast_to(rows[i : i + 1, :], (8, LANES)) - iota8
            high = jnp.zeros((8, LANES), jnp.float32)
            low = high
            for k in range(depth // 8):
                hit = wanted == 8 * k
                at, cols = 8 * k, slice(i * LANES, (i + 1) * LANES)
                high = jnp.where(hit, spread[at : at + 8, cols], high)
                low = jnp.where(hit, spread[depth + at : depth + at + 8, cols], low)
            found.append(jnp.sum(high + low, axis=0, keepdims=True))
        return jnp.concatenate(found, axis=0)

    def pick(lanes, rows, lines, found):
        for k, line in lines:
            moved = jnp.take_along_axis(
                jnp.broadcast_to(line, (8, LANES)), lanes, axis=1, mode="promise_in_bounds"
            )
            found = jnp.where(rows == k, moved, found)
        return found

    def parts_of(values):
        high = values.astype(jnp.bfloat16).astype(jnp.float32)
        return high, values - high

    def against(placed, g):
        return lax.dot_general(
            placed,
            onehot[g, :, 0 : placed.shape[1]],
            (((1,), (1,)), ((), ())),
            preferred_element_type=jnp.float32,
        )

    def scatter(g, values, base, depth, count=8):
        rows = row_of[group(g), :] - base
        high, low = parts_of(values)
        row_iota = lax.broadcasted_iota(jnp.int32, (depth, LANES), 0)
        columns = []
        for i in range(count):
            hit = rows[i : i + 1, :] == row_iota
            upper_part = jnp.where(hit, high[i : i + 1, :], 0.0).astype(jnp.bfloat16)
            lower_part = jnp.where(hit, low[i : i + 1, :], 0.0).astype(jnp.bfloat16)
            columns.append(jnp.concatenate([upper_part, lower_part], axis=0))
        return against(jnp.concatenate(columns, axis=1), g)

    def scatter_far(g, values):
        rows = row_of[group(g), :] - own_rows
        high, low = parts_of(values)
        row_iota = lax.broadcasted_iota(jnp.int32, (ghost_rows, LANES), 0)
        con_iota = lax.broadcasted_iota(jnp.int32, (2 * con_pad, LANES), 0)
        con_row = ghost_rows + lax.rem(con_iota, con_pad)
        columns = []
        for i in range(8):
            one = rows[i : i + 1, :]
            hit = one == row_iota
            con_hit = one == con_row
            top, bottom = high[i : i + 1, :], low[i : i + 1, :]
            both = jnp.where(con_iota < con_pad, top, bottom)
            columns.append(
                jnp.concatenate(
                    [
                        jnp.where(hit, top, 0.0).astype(jnp.bfloat16),
                        jnp.where(hit, bottom, 0.0).astype(jnp.bfloat16),
                        jnp.where(con_hit, both, 0.0).astype(jnp.bfloat16),
                    ],
                    axis=0,
                )
            )
        placed = jnp.concatenate(columns, axis=1)
        return lax.dot_general(
            onehot[g], placed, (((1,), (1,)), ((), ())), preferred_element_type=jnp.float32
        )

    def folded(both):
        depth = both.shape[0] // 2
        return both[0:depth] + both[depth : 2 * depth]

    def store(table, value):
        high, low = split(value)
        size = value.shape[0]
        table[0:size, :] = high
        table[size : 2 * size, :] = low

    def out_copy(turn, side, k):
        j = side * half + k
        return pltpu.make_async_remote_copy(
            src_ref=out_src.at[turn, j],
            dst_ref=out_dst.at[turn, j],
            send_sem=out_send.at[side],
            recv_sem=out_recv.at[side, int(k == slow)],
            device_id=place(ring_peer(offset(side, k))),
            device_id_type=MESH,
        )

    def back_copy(turn, side, k):
        j = side * half + k
        return pltpu.make_async_remote_copy(
            src_ref=back_src.at[turn, j],
            dst_ref=back_dst.at[turn, j],
            send_sem=back_send.at[side],
            recv_sem=back_recv.at[side, int(k == slow)],
            device_id=place(ring_peer(-offset(side, k))),
            device_id_type=MESH,
        )

    def near_copy(turn, step):
        return pltpu.make_async_remote_copy(
            src_ref=part.at[turn],
            dst_ref=first_buf.at[turn, near_id],
            send_sem=first_send.at[turn],
            recv_sem=first_recv.at[turn],
            device_id=place(near_peer(step)),
            device_id_type=MESH,
        )

    def far_copy(turn, step):
        return pltpu.make_async_remote_copy(
            src_ref=mid_part.at[turn],
            dst_ref=second_buf.at[turn, far_id],
            send_sem=second_send.at[turn],
            recv_sem=second_recv.at[turn],
            device_id=place(far_peer(step)),
            device_id_type=MESH,
        )

    out_ends = (out_src, out_dst, out_send, out_recv)
    back_ends = (back_src, back_dst, back_send, back_recv)

    def list_values(turn, side, q):
        lines = [(r, own_values[r : r + 1, :]) for r in range(own_rows)]
        at = group(list_base + side * side_groups + q)
        zero = jnp.zeros((8, LANES), jnp.float32)
        found = pick(lane_of[2 * turn, at, :], row_of[at, :], lines, zero)
        for r in range(per_group):
            j = side * half + q * per_group + r
            out_src[turn, j] = found[r * block_rows : (r + 1) * block_rows]

    def arrived(turn, side, mixed, which):
        source = turn
        if mixed is not None:
            source = ITERS
            for k in which:
                j = side * half + k
                out_dst[source, j] = mixed(*[out_dst[t, j] for t in range(turn + 1)])
        return [
            (k * block_rows + r, out_dst[source, side * half + k, r : r + 1, :])
            for k in which
            for r in range(block_rows)
        ]

    def settle(ref, sem):
        pltpu.make_async_copy(ref, ref, sem).wait()

    def take_most(ends, turn, side):
        if half > 1:
            settle(ends[1].at[turn, pl.ds(side * half, half - 1)], ends[3].at[side, 0])

    def take_slow(ends, turn, side):
        settle(ends[1].at[turn, pl.ds(side * half, 1)], ends[3].at[side, 1])

    def sent(ends, turn, side):
        settle(ends[0].at[turn, pl.ds(side * half, half)], ends[2].at[side])

    def begin_apply(turn, vector):
        own_values[...] = vector
        for side in (sent_first, upper):
            for q in group_order:
                list_values(turn, side, q)
                if turn == 0 and side is sent_first and q == slow_group:
                    pl.semaphore_wait(barrier, len(peers))
                for k in block_order:
                    if k // per_group == q:
                        out_copy(turn, side, k).start()

    def apply(turn, vector, mixed, begin, middle):
        store(own_table, vector)

        def take_own(g, carry):
            cell_buf[group(g), :] = gather(g, own_table)
            return carry

        lax.fori_loop(0, work_groups, take_own, 0, unroll=UNROLL)

        early, late = sent_first, upper
        take_most(out_ends, turn, early)
        take_slow(out_ends, turn, early)
        lines = arrived(turn, early, mixed, range(half))
        base = own_rows + early * side_rows
        for g in range(work_groups):
            at = slice(8 * g, 8 * g + 8)
            cell_buf[at, :] = pick(lane_of[2 * turn, at, :], row_of[at, :] - base, lines, cell_buf[at, :])

        base = own_rows + late * side_rows
        if half > 1:
            take_most(out_ends, turn, late)
            lines = arrived(turn, late, mixed, block_order[1:])
            for g in range(work_groups):
                at = slice(8 * g, 8 * g + 8)
                cell_buf[at, :] = pick(lane_of[2 * turn + 1, at, :], row_of[at, :] - base, lines, cell_buf[at, :])

        take_slow(out_ends, turn, late)
        lines = arrived(turn, late, mixed, [slow])
        resolved = []
        for h in range(con_rows):
            at, to = slice(8 * (con_base + h), 8 * (con_base + h) + 8), slice(8 * h, 8 * h + 8)
            found = pick(lane_of[2 * turn + 1, at, :], row_of[at, :] - base, lines, cell_buf[at, :])
            resolved.append((h, jnp.sum(weights[to, :] * found, axis=0, keepdims=True)))
        found = []
        for g in range(cell_groups):
            at = slice(8 * g, 8 * g + 8)
            found.append(pick(lane_of[2 * turn + 1, at, :], row_of[at, :] - base, lines, cell_buf[at, :]))
        for g in range(cell_groups):
            at = slice(8 * g, 8 * g + 8)
            rows = row_of[at, :] - (own_rows + ghost_rows)
            found[g] = pick(lane_of[2 * turn + 1, at, :], rows, resolved, found[g])
        nodal = jnp.concatenate(found, axis=0)
        contrib = scale * jnp.dot(
            stiff_ref[...],
            nodal,
            precision=lax.Precision.HIGHEST,
            preferred_element_type=jnp.float32,
        )
        cell_buf[0:cell_rows, :] = contrib
        weighted = reaction_ref[...] * vector
        energy = jnp.sum(nodal * contrib, axis=0, keepdims=True)
        energy = energy + jnp.sum(weighted * vector, axis=0, keepdims=True)
        begin(energy)


        def give_all_far():
            total = jnp.zeros((LANES, 2 * far_rows), jnp.float32)
            for g in range(cell_groups):
                total = total + scatter_far(g, cell_buf[8 * g : 8 * g + 8, :])
            far_acc[...] = total

        apart(give_all_far)
        total = jnp.transpose(far_acc[...])
        spread = total[0:ghost_rows] + total[ghost_rows : 2 * ghost_rows]
        summed = folded(total[2 * ghost_rows : 2 * far_rows])
        for h in range(con_rows):
            shares = weights[8 * h : 8 * h + 8, :] * summed[h : h + 1]
            cell_buf[8 * (con_base + h) : 8 * (con_base + h) + 8, :] = shares

        def give_con():
            total = jnp.zeros((2 * ghost_rows, LANES), jnp.float32)
            for h in range(con_rows):
                values = cell_buf[8 * (con_base + h) : 8 * (con_base + h) + 8, :]
                total = total + scatter(con_base + h, values, own_rows, ghost_rows, nodes)
            con_acc[...] = total

        apart(give_con)
        spread = spread + folded(con_acc[...])
        for j in range(blocks):
            back_src[turn, j] = spread[j * block_rows : (j + 1) * block_rows]
        for side in (late, early):
            for k in block_order:
                back_copy(turn, side, k).start()
        middle()
        own_acc[...] = jnp.zeros_like(own_acc)

        def give_own(g, carry):
            own_acc[...] += scatter(g, cell_buf[group(g), :], 0, own_rows)
            return carry

        lax.fori_loop(0, work_groups, give_own, 0, unroll=UNROLL)
        def give_lists(side, which):
            def work():
                both = own_acc[...]
                for q in which:
                    j = side * half + q * per_group
                    values = jnp.concatenate([back_dst[turn, j + r] for r in range(per_group)], axis=0)
                    both = both + scatter(list_base + side * side_groups + q, values, 0, own_rows)
                own_acc[...] = both

            apart(work)

        sent(out_ends, turn, early)
        sent(out_ends, turn, late)
        take_most(back_ends, turn, late)
        take_slow(back_ends, turn, late)
        give_lists(late, group_order)
        take_most(back_ends, turn, early)
        if side_groups > 1:
            give_lists(early, group_order[1:])
        take_slow(back_ends, turn, early)
        give_lists(early, group_order[:1])
        sent(back_ends, turn, late)
        sent(back_ends, turn, early)
        both = own_acc[...]
        return folded(both) + weighted

    def dot(one, two):
        return jnp.sum(one * two, axis=0, keepdims=True)

    lane = lax.broadcasted_iota(jnp.int32, (1, LANES), 1)
    width = LANES // SUMS

    def sums_start(turn, parts):
        total = jnp.sum(jnp.concatenate(parts, axis=0), axis=1, keepdims=True)
        mine = jnp.zeros((1, LANES), jnp.float32)
        for k in range(len(parts)):
            mine = jnp.where(lax.div(lane, width) == k, total[k : k + 1], mine)
        part[turn] = mine
        first_buf[turn, near_id] = mine

    def sums_send(turn):
        for step in range(1, near):
            near_copy(turn, step).start()

    def near_total(turn):
        others = pl.ds(0, near - 1)
        settle(first_buf.at[turn, others], first_send.at[turn])
        settle(first_buf.at[turn, others], first_recv.at[turn])
        mine = first_buf[turn, 0]
        for k in range(1, near):
            mine = mine + first_buf[turn, k]
        return mine

    def sums_middle(turn):
        sums_send(turn)
        if far == 1:
            return
        mine = near_total(turn)
        mid_part[turn] = mine
        second_buf[turn, far_id] = mine
        for step in range(1, far):
            far_copy(turn, step).start()

    def sums_end(turn):
        if far == 1:
            total = near_total(turn)
        else:
            others = pl.ds(0, far - 1)
            settle(second_buf.at[turn, others], second_send.at[turn])
            settle(second_buf.at[turn, others], second_recv.at[turn])
            total = second_buf[turn, 0]
            for k in range(1, far):
                total = total + second_buf[turn, k]
        return [total[:, k * width : k * width + 1] for k in range(SUMS)]

    loads[0].wait()
    loads[6].wait()
    for side in range(2):
        for k in range(half):
            j = side * half + k
            other = me + offset(side, k)
            inside = jnp.logical_and(other >= 0, other < count)
            for q in range(block_rows):
                at = list_base * 8 + j * block_rows + q
                put(at, lists_ref[j : j + 1, q * LANES : (q + 1) * LANES], inside)
    start = right_ref[...]
    begin_apply(0, start)
    for i in order[2:]:
        loads[i].wait()
    for copy in range(2 * ITERS):
        lane_of[copy, points:cell_rows, :] = jnp.zeros((cell_rows - points, LANES), jnp.int32)
    row_of[points:cell_rows, :] = jnp.full((cell_rows - points, LANES), -1, jnp.int32)
    slots = cells_ref[...]
    put(0, slots, held(slots))
    weights[...] = jnp.zeros_like(weights)
    for h in range(con_rows):
        at = (con_base + h) * 8
        for copy in range(2 * ITERS):
            lane_of[copy, at : at + 8, :] = jnp.zeros((8, LANES), jnp.int32)
        row_of[at : at + 8, :] = jnp.full((8, LANES), -1, jnp.int32)
        slots = masters_ref[:, h * LANES : (h + 1) * LANES]
        put(at, slots, held(slots))
        chosen = rows_ref[h : h + 1, :]
        for k in range(nodes):
            weight = jnp.zeros((1, LANES), jnp.float32)
            for t in range(interp.shape[0]):
                weight = jnp.where(chosen == t, float(interp[t, k]), weight)
            weights[h * 8 + k : h * 8 + k + 1, :] = weight
    lax.fori_loop(0, onehot.shape[0], build, 0)
    scale = jnp.exp2(-level_ref[...].astype(jnp.float32))

    first = apply(0, start, None, lambda energy: None, lambda: None)
    begin_apply(1, first)
    known = [dot(start, start), dot(start, first), dot(first, first)]
    second = apply(
        1,
        first,
        None,
        lambda energy: sums_start(0, known + [energy]),
        lambda: sums_middle(0),
    )
    begin_apply(2, second)
    m0, m1, m2, m3 = sums_end(0)
    step0 = m0 / m1
    norm1 = m0 - 2.0 * step0 * m1 + step0 * step0 * m2
    product1 = m1 - 2.0 * step0 * m2 + step0 * step0 * m3
    ratio1 = norm1 / m0
    step1 = norm1 / (product1 - ratio1 * norm1 / step0)

    def next_residual(zeroth, once, twice):
        before = zeroth - step0 * once
        along = once - step0 * twice + ratio1 * once
        return before, along, before - step1 * along

    before, applied_dir, residual = next_residual(start, first, second)
    direction = before + ratio1 * start
    answer = step0 * start + step1 * direction
    square = dot(residual, residual)
    applied = apply(
        2,
        residual,
        lambda *held: next_residual(*held)[2],
        lambda energy: sums_start(1, [square, energy]),
        lambda: sums_middle(1),
    )
    norm2, product2, unused_a, unused_b = sums_end(1)
    ratio2 = norm2 / norm1
    step2 = norm2 / (product2 - ratio2 * norm2 / step1)
    answer_ref[...] = answer
    ahead_ref[...] = residual + ratio2 * direction
    residual_ref[...] = residual
    applied_ref[...] = applied + ratio2 * applied_dir
    step_ref[...] = jnp.broadcast_to(step2, step_ref.shape)


def phases(count):
    if count <= 64:
        return count, 1
    near = 1
    while near * near < count:
        near *= 2
    return near, count // near


def on_device(shape, right_side, reaction, cell_slots, cell_level, con_masters, con_rows, send_lists):
    interp, stiffness = tables()
    own = right_side.shape[0]
    own_rows = own // LANES
    blocks, listed = send_lists.shape
    block_rows = listed // LANES
    con_tiles = con_rows.shape[0] // LANES
    points = cell_slots.shape[0]
    cell_rows = round_up(points, 8)
    far_rows = blocks * block_rows + round_up(con_tiles, 8)
    groups = cell_rows // 8 + blocks * block_rows // 8 + con_tiles
    padded = np.zeros((cell_rows, cell_rows), np.float32)
    padded[:points, :points] = stiffness
    count = shape[0] * shape[1]
    near, far = phases(count)
    operands = [
        right_side.reshape(own_rows, LANES),
        reaction.reshape(own_rows, LANES),
        cell_slots,
        cell_level.reshape(1, -1),
        con_masters,
        con_rows.reshape(con_tiles, LANES),
        send_lists,
        jnp.asarray(padded),
    ]
    exchange = pltpu.VMEM((ITERS, blocks, block_rows, LANES), jnp.float32)
    landing = pltpu.VMEM((ITERS + 1, blocks, block_rows, LANES), jnp.float32)
    tile = pltpu.VMEM((own_rows, LANES), jnp.float32)
    line = pltpu.VMEM((1, LANES), jnp.float32)
    answer, ahead, residual, applied, step = pl.pallas_call(
        functools.partial(kernel, shape, interp),
        out_shape=(tile, tile, tile, tile, line),
        in_specs=[pl.BlockSpec(memory_space=pl.ANY)] * 8,
        out_specs=(pl.BlockSpec(memory_space=pltpu.VMEM),) * 5,
        scratch_shapes=[
            *[pltpu.VMEM(value.shape, value.dtype) for value in operands],
            pltpu.SemaphoreType.DMA((len(operands),)),
            pltpu.VMEM((own_rows, LANES), jnp.float32),
            pltpu.VMEM((2 * own_rows, LANES), jnp.bfloat16),
            pltpu.VMEM((groups, LANES, 8 * LANES), jnp.bfloat16),
            pltpu.VMEM((2 * ITERS, groups * 8, LANES), jnp.int32),
            pltpu.VMEM((groups * 8, LANES), jnp.int32),
            pltpu.VMEM((con_tiles * 8, LANES), jnp.float32),
            pltpu.VMEM((cell_rows + 8 * con_tiles, LANES), jnp.float32),
            pltpu.VMEM((2 * own_rows, LANES), jnp.float32),
            pltpu.VMEM((LANES, 2 * far_rows), jnp.float32),
            pltpu.VMEM((2 * blocks * block_rows, LANES), jnp.float32),
            exchange,
            landing,
            exchange,
            exchange,
            pltpu.VMEM((ROUNDS, 1, LANES), jnp.float32),
            pltpu.VMEM((ROUNDS, near, 1, LANES), jnp.float32),
            pltpu.VMEM((ROUNDS, 1, LANES), jnp.float32),
            pltpu.VMEM((ROUNDS, far, 1, LANES), jnp.float32),
            pltpu.SemaphoreType.DMA((2,)),
            pltpu.SemaphoreType.DMA((2, 2)),
            pltpu.SemaphoreType.DMA((2,)),
            pltpu.SemaphoreType.DMA((2, 2)),
            pltpu.SemaphoreType.DMA((ROUNDS,)),
            pltpu.SemaphoreType.DMA((ROUNDS,)),
            pltpu.SemaphoreType.DMA((ROUNDS,)),
            pltpu.SemaphoreType.DMA((ROUNDS,)),
        ],
        compiler_params=pltpu.CompilerParams(
            collective_id=0, has_side_effects=True, vmem_limit_bytes=60 * 1024 * 1024
        ),
    )(*operands)
    scale = step[0, 0]
    return (
        (answer + scale * ahead).reshape(own),
        (residual - scale * applied).reshape(own),
    )


def solution(mesh):
    placed = (
        P(("gx", "gy")),
        P(("gx", "gy")),
        P(None, ("gx", "gy")),
        P(("gx", "gy")),
        P(None, ("gx", "gy")),
        P(("gx", "gy")),
        P(None, ("gx", "gy")),
    )
    return jax.shard_map(
        functools.partial(on_device, (mesh.shape["gx"], mesh.shape["gy"])),
        mesh=mesh,
        in_specs=placed,
        out_specs=(P(("gx", "gy")), P(("gx", "gy"))),
        check_vma=False,
    )
```

```python
import functools

import jax
import jax.numpy as jnp
import numpy as np
from jax import lax
from jax.experimental import pallas as pl
from jax.experimental.pallas import tpu as pltpu
from jax.sharding import PartitionSpec as P

ITERS = 3
LANES = 128
SUMS = 4
ROUNDS = 2
UNROLL = 9
MESH = pl.DeviceIdType.MESH


def lagrange(node_list, points):
    node_count = len(node_list)
    values = np.ones((len(points), node_count))
    derivs = np.zeros((len(points), node_count))
    for basis_node in range(node_count):
        for other_node in range(node_count):
            if other_node != basis_node:
                values[:, basis_node] = (
                    values[:, basis_node]
                    * (points - node_list[other_node])
                    / (node_list[basis_node] - node_list[other_node])
                )
        for skipped in range(node_count):
            if skipped != basis_node:
                product_term = np.ones(len(points)) / (node_list[basis_node] - node_list[skipped])
                for other_node in range(node_count):
                    if other_node != basis_node and other_node != skipped:
                        product_term = (
                            product_term
                            * (points - node_list[other_node])
                            / (node_list[basis_node] - node_list[other_node])
                        )
                derivs[:, basis_node] = derivs[:, basis_node] + product_term
    return (values, derivs)


def tables():
    gll_offset = np.sqrt(3.0 / 7.0)
    lobatto = np.array([0.0, (1.0 - gll_offset) / 2.0, 0.5, (1.0 + gll_offset) / 2.0, 1.0])
    inner_point = np.sqrt(5.0 - 2.0 * np.sqrt(10.0 / 7.0)) / 3.0
    outer_point = np.sqrt(5.0 + 2.0 * np.sqrt(10.0 / 7.0)) / 3.0
    inner_weight = (322.0 + 13.0 * np.sqrt(70.0)) / 900.0
    outer_weight = (322.0 - 13.0 * np.sqrt(70.0)) / 900.0
    points = np.array([-outer_point, -inner_point, 0.0, inner_point, outer_point])
    gauss_weights = np.array(
        [outer_weight, inner_weight, 128.0 / 225.0, inner_weight, outer_weight]
    )
    points = (points + 1.0) / 2.0
    gauss_weights = gauss_weights / 2.0
    shapes, slopes = lagrange(lobatto, points)
    fine_points = np.concatenate([lobatto / 2.0, (1.0 + lobatto) / 2.0])
    interp, unused_slopes = lagrange(lobatto, fine_points)
    quad_weights = np.kron(gauss_weights, np.kron(gauss_weights, gauss_weights))
    grad_x = np.kron(slopes, np.kron(shapes, shapes))
    grad_y = np.kron(shapes, np.kron(slopes, shapes))
    grad_z = np.kron(shapes, np.kron(shapes, slopes))
    stiffness = np.zeros((125, 125))
    for gradient in (grad_x, grad_y, grad_z):
        stiffness = stiffness + gradient.T @ (quad_weights[:, None] * gradient)
    return (interp.astype(np.float32), stiffness.astype(np.float32))


def round_up(value, step):
    return -(-value // step) * step


def split(value):
    high = value.astype(jnp.bfloat16)
    low = (value - high.astype(jnp.float32)).astype(jnp.bfloat16)
    return high, low


def kernel(
    shape,
    interp,
    *refs,
):
    inputs, refs = refs[:8], refs[8:]
    answer_ref, ahead_ref, residual_ref, applied_ref, step_ref = refs[:5]
    staged, refs = refs[5:13], refs[13:]
    right_ref, reaction_ref, cells_ref, level_ref, masters_ref, rows_ref, lists_ref, stiff_ref = staged
    (
    load_sem,
    own_values,
    own_table,
    onehot,
    lane_of,
    row_of,
    weights,
    cell_buf,
    own_acc,
    far_acc,
    con_acc,
    out_src,
    out_dst,
    back_src,
    back_dst,
    part,
    first_buf,
    mid_part,
    second_buf,
    out_send,
    out_recv,
    back_send,
    back_recv,
    first_send,
    first_recv,
    second_send,
    second_recv,
    ) = refs
    loads = [
        pltpu.make_async_copy(source, target, load_sem.at[i])
        for i, (source, target) in enumerate(zip(inputs, staged))
    ]
    order = [0, 6, 2, 4, 5, 3, 1, 7]
    for i in order:
        loads[i].start()
    nx, ny = shape
    count = nx * ny
    inner = lax.axis_index("gy")
    me = lax.axis_index("gx") * ny + inner
    upper = lax.div(2 * inner, ny)

    def place(rank):
        return (lax.div(rank, ny), lax.rem(rank, ny))

    blocks, listed = lists_ref.shape
    half = blocks // 2
    own_rows = right_ref.shape[0]
    block_rows = listed // LANES
    ghost_rows = blocks * block_rows
    side_rows = half * block_rows
    con_rows = rows_ref.shape[0]
    con_pad = round_up(con_rows, 8)
    far_rows = ghost_rows + con_pad
    nodes = masters_ref.shape[0]
    points = cells_ref.shape[0]
    cell_rows = round_up(points, 8)
    cell_groups = cell_rows // 8
    list_groups = ghost_rows // 8
    side_groups = list_groups // 2
    per_group = 8 // block_rows
    con_base = cell_groups
    work_groups = cell_groups + con_rows
    list_base = work_groups
    near, far = phases(count)
    near_id, far_id = lax.rem(me, near), lax.div(me, near)
    sent_first = 1 - upper
    slow = min(1, half - 1)
    slow_group = slow // per_group
    group_order = [slow_group] + [q for q in range(side_groups) if q != slow_group]
    block_order = [slow] + [k for k in range(half) if k != slow]

    def offset(side, k):
        return (k + 1) * (1 - 2 * side)

    def near_peer(step):
        return far_id * near + lax.rem(near_id + step, near)

    def far_peer(step):
        return lax.rem(far_id + step, far) * near + near_id

    def ring_peer(distance):
        return lax.rem(me + distance + count, count)

    barrier = pltpu.get_barrier_semaphore()
    peers = []
    if far > 1:
        peers += [ring_peer(offset(side, k)) for side in range(2) for k in range(half)]
    peers += [near_peer(step) for step in range(1, near)]
    peers += [far_peer(step) for step in range(1, far)]
    for peer in peers:
        pl.semaphore_signal(barrier, inc=1, device_id=place(peer), device_id_type=MESH)

    def put(at, slots, shown):
        size = slots.shape[0]
        for copy in range(2 * ITERS):
            lane_of[copy, at : at + size, :] = lax.rem(slots, LANES)
        row_of[at : at + size, :] = jnp.where(shown, lax.div(slots, LANES), -1)

    def held(slots):
        rows = lax.div(slots, LANES) - own_rows
        shown = jnp.full(slots.shape, True)
        for side in range(2):
            for k in range(half):
                other = me - offset(side, k)
                low = (side * half + k) * block_rows
                outside = jnp.logical_or(other < 0, other >= count)
                hidden = jnp.logical_and(rows >= low, rows < low + block_rows)
                shown = jnp.logical_and(shown, jnp.logical_not(jnp.logical_and(hidden, outside)))
        return shown

    lane_iota = lax.broadcasted_iota(jnp.int32, (LANES, LANES), 0)

    def build(g, carry):
        lanes = lane_of[0, pl.ds(pl.multiple_of(g * 8, 8), 8), :]
        for i in range(8):
            hit = jnp.where(lanes[i : i + 1, :] == lane_iota, 1.0, 0.0)
            onehot[g, :, i * LANES : (i + 1) * LANES] = hit.astype(jnp.bfloat16)
        return carry

    iota8 = lax.broadcasted_iota(jnp.int32, (8, LANES), 0)

    once = 1 + lax.div(inner, ny)

    def apart(work):
        def body(i, carry):
            work()
            return carry

        lax.fori_loop(0, once, body, 0)

    def group(g):
        return pl.ds(pl.multiple_of(g * 8, 8), 8)

    def gather(g, table):
        depth = table.shape[0] // 2
        spread = jnp.dot(table[...], onehot[g], preferred_element_type=jnp.float32)
        rows = row_of[group(g), :]
        found = []
        for i in range(8):
            wanted = jnp.broadcast_to(rows[i : i + 1, :], (8, LANES)) - iota8
            high = jnp.zeros((8, LANES), jnp.float32)
            low = high
            for k in range(depth // 8):
                hit = wanted == 8 * k
                at, cols = 8 * k, slice(i * LANES, (i + 1) * LANES)
                high = jnp.where(hit, spread[at : at + 8, cols], high)
                low = jnp.where(hit, spread[depth + at : depth + at + 8, cols], low)
            found.append(jnp.sum(high + low, axis=0, keepdims=True))
        return jnp.concatenate(found, axis=0)

    def pick(lanes, rows, lines, found):
        for k, line in lines:
            moved = jnp.take_along_axis(
                jnp.broadcast_to(line, (8, LANES)), lanes, axis=1, mode="promise_in_bounds"
            )
            found = jnp.where(rows == k, moved, found)
        return found

    def parts_of(values):
        high = values.astype(jnp.bfloat16).astype(jnp.float32)
        return high, values - high

    def against(placed, g, first):
        return lax.dot_general(
            placed,
            onehot[g, :, first * LANES : first * LANES + placed.shape[1]],
            (((1,), (1,)), ((), ())),
            preferred_element_type=jnp.float32,
        )

    def scatter(g, values, base, depth, first=0):
        rows = row_of[group(g), :] - base
        high, low = parts_of(values)
        row_iota = lax.broadcasted_iota(jnp.int32, (depth, LANES), 0)
        columns = []
        for i in range(values.shape[0]):
            hit = rows[first + i : first + i + 1, :] == row_iota
            upper_part = jnp.where(hit, high[i : i + 1, :], 0.0).astype(jnp.bfloat16)
            lower_part = jnp.where(hit, low[i : i + 1, :], 0.0).astype(jnp.bfloat16)
            columns.append(jnp.concatenate([upper_part, lower_part], axis=0))
        return against(jnp.concatenate(columns, axis=1), g, first)

    def scatter_far(g, values):
        rows = row_of[group(g), :] - own_rows
        high, low = parts_of(values)
        row_iota = lax.broadcasted_iota(jnp.int32, (ghost_rows, LANES), 0)
        con_iota = lax.broadcasted_iota(jnp.int32, (2 * con_pad, LANES), 0)
        con_row = ghost_rows + lax.rem(con_iota, con_pad)
        columns = []
        for i in range(8):
            one = rows[i : i + 1, :]
            hit = one == row_iota
            con_hit = one == con_row
            top, bottom = high[i : i + 1, :], low[i : i + 1, :]
            both = jnp.where(con_iota < con_pad, top, bottom)
            columns.append(
                jnp.concatenate(
                    [
                        jnp.where(hit, top, 0.0).astype(jnp.bfloat16),
                        jnp.where(hit, bottom, 0.0).astype(jnp.bfloat16),
                        jnp.where(con_hit, both, 0.0).astype(jnp.bfloat16),
                    ],
                    axis=0,
                )
            )
        placed = jnp.concatenate(columns, axis=1)
        return lax.dot_general(
            onehot[g], placed, (((1,), (1,)), ((), ())), preferred_element_type=jnp.float32
        )

    def folded(both):
        depth = both.shape[0] // 2
        return both[0:depth] + both[depth : 2 * depth]

    def store(table, value):
        high, low = split(value)
        size = value.shape[0]
        table[0:size, :] = high
        table[size : 2 * size, :] = low

    def out_copy(turn, side, k):
        j = side * half + k
        return pltpu.make_async_remote_copy(
            src_ref=out_src.at[turn, j],
            dst_ref=out_dst.at[turn, j],
            send_sem=out_send.at[side],
            recv_sem=out_recv.at[side, int(k == slow)],
            device_id=place(ring_peer(offset(side, k))),
            device_id_type=MESH,
        )

    def back_copy(turn, side, k):
        j = side * half + k
        return pltpu.make_async_remote_copy(
            src_ref=back_src.at[turn, j],
            dst_ref=back_dst.at[turn, j],
            send_sem=back_send.at[side],
            recv_sem=back_recv.at[side, int(k == slow)],
            device_id=place(ring_peer(-offset(side, k))),
            device_id_type=MESH,
        )

    def near_copy(turn, step):
        return pltpu.make_async_remote_copy(
            src_ref=part.at[turn],
            dst_ref=first_buf.at[turn, near_id],
            send_sem=first_send.at[turn],
            recv_sem=first_recv.at[turn],
            device_id=place(near_peer(step)),
            device_id_type=MESH,
        )

    def far_copy(turn, step):
        return pltpu.make_async_remote_copy(
            src_ref=mid_part.at[turn],
            dst_ref=second_buf.at[turn, far_id],
            send_sem=second_send.at[turn],
            recv_sem=second_recv.at[turn],
            device_id=place(far_peer(step)),
            device_id_type=MESH,
        )

    out_ends = (out_src, out_dst, out_send, out_recv)
    back_ends = (back_src, back_dst, back_send, back_recv)

    def list_values(turn, side, q):
        lines = [(r, own_values[r : r + 1, :]) for r in range(own_rows)]
        at = group(list_base + side * side_groups + q)
        zero = jnp.zeros((8, LANES), jnp.float32)
        found = pick(lane_of[2 * turn, at, :], row_of[at, :], lines, zero)
        for r in range(per_group):
            j = side * half + q * per_group + r
            out_src[turn, j] = found[r * block_rows : (r + 1) * block_rows]

    def arrived(turn, side, mixed, which):
        source = turn
        if mixed is not None:
            source = ITERS
            for k in which:
                j = side * half + k
                out_dst[source, j] = mixed(*[out_dst[t, j] for t in range(turn + 1)])
        return [
            (k * block_rows + r, out_dst[source, side * half + k, r : r + 1, :])
            for k in which
            for r in range(block_rows)
        ]

    def settle(ref, sem):
        pltpu.make_async_copy(ref, ref, sem).wait()

    def take_most(ends, turn, side):
        if half > 1:
            settle(ends[1].at[turn, pl.ds(side * half, half - 1)], ends[3].at[side, 0])

    def take_slow(ends, turn, side):
        settle(ends[1].at[turn, pl.ds(side * half, 1)], ends[3].at[side, 1])

    def sent(ends, turn, side):
        settle(ends[0].at[turn, pl.ds(side * half, half)], ends[2].at[side])

    def begin_apply(turn, vector):
        own_values[...] = vector
        for side in (sent_first, upper):
            for q in group_order:
                list_values(turn, side, q)
                if turn == 0 and side is sent_first and q == slow_group:
                    pl.semaphore_wait(barrier, len(peers))
                for k in block_order:
                    if k // per_group == q:
                        out_copy(turn, side, k).start()

    def apply(turn, vector, mixed, begin, middle):
        store(own_table, vector)

        def take_own(g, carry):
            cell_buf[group(g), :] = gather(g, own_table)
            return carry

        lax.fori_loop(0, work_groups, take_own, 0, unroll=UNROLL)

        early, late = sent_first, upper
        take_most(out_ends, turn, early)
        take_slow(out_ends, turn, early)
        lines = arrived(turn, early, mixed, range(half))
        base = own_rows + early * side_rows
        for g in range(work_groups):
            at = slice(8 * g, 8 * g + 8)
            cell_buf[at, :] = pick(lane_of[2 * turn, at, :], row_of[at, :] - base, lines, cell_buf[at, :])

        base = own_rows + late * side_rows
        if half > 1:
            take_most(out_ends, turn, late)
            lines = arrived(turn, late, mixed, block_order[1:])
            for g in range(work_groups):
                at = slice(8 * g, 8 * g + 8)
                cell_buf[at, :] = pick(lane_of[2 * turn + 1, at, :], row_of[at, :] - base, lines, cell_buf[at, :])

        take_slow(out_ends, turn, late)
        lines = arrived(turn, late, mixed, [slow])
        resolved = []
        for h in range(con_rows):
            at, to = slice(8 * (con_base + h), 8 * (con_base + h) + 8), slice(8 * h, 8 * h + 8)
            found = pick(lane_of[2 * turn + 1, at, :], row_of[at, :] - base, lines, cell_buf[at, :])
            resolved.append((h, jnp.sum(weights[to, :] * found, axis=0, keepdims=True)))
        found = []
        for g in range(cell_groups):
            at = slice(8 * g, 8 * g + 8)
            lanes, rows = lane_of[2 * turn + 1, at, :], row_of[at, :]
            part_found = pick(lanes, rows - base, lines, cell_buf[at, :])
            found.append(pick(lanes, rows - (own_rows + ghost_rows), resolved, part_found))
        nodal = jnp.concatenate(found, axis=0)
        contrib = scale * jnp.dot(
            stiff_ref[...],
            nodal,
            precision=lax.Precision.HIGHEST,
            preferred_element_type=jnp.float32,
        )
        cell_buf[0:cell_rows, :] = contrib
        weighted = reaction_ref[...] * vector
        energy = jnp.sum(nodal * contrib, axis=0, keepdims=True)
        energy = energy + jnp.sum(weighted * vector, axis=0, keepdims=True)
        begin(energy)


        def give_all_far():
            total = jnp.zeros((LANES, 2 * far_rows), jnp.float32)
            for g in range(cell_groups):
                total = total + scatter_far(g, cell_buf[8 * g : 8 * g + 8, :])
            far_acc[...] = total

        apart(give_all_far)
        total = jnp.transpose(far_acc[...])
        spread = total[0:ghost_rows] + total[ghost_rows : 2 * ghost_rows]
        summed = folded(total[2 * ghost_rows : 2 * far_rows])
        for h in range(con_rows):
            shares = weights[8 * h : 8 * h + 8, :] * summed[h : h + 1]
            cell_buf[8 * (con_base + h) : 8 * (con_base + h) + 8, :] = shares

        def give_con():
            total = jnp.zeros((2 * ghost_rows, LANES), jnp.float32)
            for h in range(con_rows):
                values = cell_buf[8 * (con_base + h) : 8 * (con_base + h) + nodes, :]
                total = total + scatter(con_base + h, values, own_rows, ghost_rows)
            con_acc[...] = total

        apart(give_con)
        spread = spread + folded(con_acc[...])
        for j in range(blocks):
            back_src[turn, j] = spread[j * block_rows : (j + 1) * block_rows]
        for side in (late, early):
            for k in block_order:
                back_copy(turn, side, k).start()
        middle()
        own_acc[...] = jnp.zeros_like(own_acc)

        def give_own(g, carry):
            own_acc[...] += scatter(g, cell_buf[group(g), :], 0, own_rows)
            return carry

        lax.fori_loop(0, work_groups, give_own, 0, unroll=UNROLL)
        def give_lists(side, which):
            def work():
                both = own_acc[...]
                for q in range(side_groups):
                    chosen = [k for k in which if k // per_group == q]
                    if not chosen:
                        continue
                    values = jnp.concatenate([back_dst[turn, side * half + k] for k in chosen], axis=0)
                    first = (chosen[0] - q * per_group) * block_rows
                    both = both + scatter(list_base + side * side_groups + q, values, 0, own_rows, first)
                own_acc[...] = both

            apart(work)

        sent(out_ends, turn, early)
        sent(out_ends, turn, late)
        take_most(back_ends, turn, late)
        take_slow(back_ends, turn, late)
        give_lists(late, range(half))
        take_most(back_ends, turn, early)
        if half > 1:
            give_lists(early, sorted(block_order[1:]))
        take_slow(back_ends, turn, early)
        give_lists(early, [slow])
        sent(back_ends, turn, late)
        sent(back_ends, turn, early)
        both = own_acc[...]
        return folded(both) + weighted

    def dot(one, two):
        return jnp.sum(one * two, axis=0, keepdims=True)

    lane = lax.broadcasted_iota(jnp.int32, (1, LANES), 1)
    width = LANES // SUMS

    def sums_start(turn, parts):
        total = jnp.sum(jnp.concatenate(parts, axis=0), axis=1, keepdims=True)
        mine = jnp.zeros((1, LANES), jnp.float32)
        for k in range(len(parts)):
            mine = jnp.where(lax.div(lane, width) == k, total[k : k + 1], mine)
        part[turn] = mine
        first_buf[turn, near_id] = mine

    def sums_send(turn):
        for step in range(1, near):
            near_copy(turn, step).start()

    def near_total(turn):
        others = pl.ds(0, near - 1)
        settle(first_buf.at[turn, others], first_send.at[turn])
        settle(first_buf.at[turn, others], first_recv.at[turn])
        mine = first_buf[turn, 0]
        for k in range(1, near):
            mine = mine + first_buf[turn, k]
        return mine

    def sums_middle(turn):
        sums_send(turn)
        if far == 1:
            return
        mine = near_total(turn)
        mid_part[turn] = mine
        second_buf[turn, far_id] = mine
        for step in range(1, far):
            far_copy(turn, step).start()

    def sums_end(turn):
        if far == 1:
            total = near_total(turn)
        else:
            others = pl.ds(0, far - 1)
            settle(second_buf.at[turn, others], second_send.at[turn])
            settle(second_buf.at[turn, others], second_recv.at[turn])
            total = second_buf[turn, 0]
            for k in range(1, far):
                total = total + second_buf[turn, k]
        return [total[:, k * width : k * width + 1] for k in range(SUMS)]

    loads[0].wait()
    loads[6].wait()
    for side in range(2):
        for k in range(half):
            j = side * half + k
            other = me + offset(side, k)
            inside = jnp.logical_and(other >= 0, other < count)
            for q in range(block_rows):
                at = list_base * 8 + j * block_rows + q
                put(at, lists_ref[j : j + 1, q * LANES : (q + 1) * LANES], inside)
    start = right_ref[...]
    begin_apply(0, start)
    for i in order[2:]:
        loads[i].wait()
    for copy in range(2 * ITERS):
        lane_of[copy, points:cell_rows, :] = jnp.zeros((cell_rows - points, LANES), jnp.int32)
    row_of[points:cell_rows, :] = jnp.full((cell_rows - points, LANES), -1, jnp.int32)
    slots = cells_ref[...]
    put(0, slots, held(slots))
    weights[...] = jnp.zeros_like(weights)
    for h in range(con_rows):
        at = (con_base + h) * 8
        for copy in range(2 * ITERS):
            lane_of[copy, at : at + 8, :] = jnp.zeros((8, LANES), jnp.int32)
        row_of[at : at + 8, :] = jnp.full((8, LANES), -1, jnp.int32)
        slots = masters_ref[:, h * LANES : (h + 1) * LANES]
        put(at, slots, held(slots))
        chosen = rows_ref[h : h + 1, :]
        for k in range(nodes):
            weight = jnp.zeros((1, LANES), jnp.float32)
            for t in range(interp.shape[0]):
                weight = jnp.where(chosen == t, float(interp[t, k]), weight)
            weights[h * 8 + k : h * 8 + k + 1, :] = weight
    lax.fori_loop(0, onehot.shape[0], build, 0)
    scale = jnp.exp2(-level_ref[...].astype(jnp.float32))

    first = apply(0, start, None, lambda energy: None, lambda: None)
    begin_apply(1, first)
    known = [dot(start, start), dot(start, first), dot(first, first)]
    second = apply(
        1,
        first,
        None,
        lambda energy: sums_start(0, known + [energy]),
        lambda: sums_middle(0),
    )
    begin_apply(2, second)
    m0, m1, m2, m3 = sums_end(0)
    step0 = m0 / m1
    norm1 = m0 - 2.0 * step0 * m1 + step0 * step0 * m2
    product1 = m1 - 2.0 * step0 * m2 + step0 * step0 * m3
    ratio1 = norm1 / m0
    step1 = norm1 / (product1 - ratio1 * norm1 / step0)

    def next_residual(zeroth, once, twice):
        before = zeroth - step0 * once
        along = once - step0 * twice + ratio1 * once
        return before, along, before - step1 * along

    before, applied_dir, residual = next_residual(start, first, second)
    direction = before + ratio1 * start
    answer = step0 * start + step1 * direction
    square = dot(residual, residual)
    applied = apply(
        2,
        residual,
        lambda *held: next_residual(*held)[2],
        lambda energy: sums_start(1, [square, energy]),
        lambda: sums_middle(1),
    )
    norm2, product2, unused_a, unused_b = sums_end(1)
    ratio2 = norm2 / norm1
    step2 = norm2 / (product2 - ratio2 * norm2 / step1)
    answer_ref[...] = answer
    ahead_ref[...] = residual + ratio2 * direction
    residual_ref[...] = residual
    applied_ref[...] = applied + ratio2 * applied_dir
    step_ref[...] = jnp.broadcast_to(step2, step_ref.shape)


def phases(count):
    if count <= 64:
        return count, 1
    near = 1
    while near * near < count:
        near *= 2
    return near, count // near


def on_device(shape, right_side, reaction, cell_slots, cell_level, con_masters, con_rows, send_lists):
    interp, stiffness = tables()
    own = right_side.shape[0]
    own_rows = own // LANES
    blocks, listed = send_lists.shape
    block_rows = listed // LANES
    con_tiles = con_rows.shape[0] // LANES
    points = cell_slots.shape[0]
    cell_rows = round_up(points, 8)
    far_rows = blocks * block_rows + round_up(con_tiles, 8)
    groups = cell_rows // 8 + blocks * block_rows // 8 + con_tiles
    padded = np.zeros((cell_rows, cell_rows), np.float32)
    padded[:points, :points] = stiffness
    count = shape[0] * shape[1]
    near, far = phases(count)
    operands = [
        right_side.reshape(own_rows, LANES),
        reaction.reshape(own_rows, LANES),
        cell_slots,
        cell_level.reshape(1, -1),
        con_masters,
        con_rows.reshape(con_tiles, LANES),
        send_lists,
        jnp.asarray(padded),
    ]
    exchange = pltpu.VMEM((ITERS, blocks, block_rows, LANES), jnp.float32)
    landing = pltpu.VMEM((ITERS + 1, blocks, block_rows, LANES), jnp.float32)
    tile = pltpu.VMEM((own_rows, LANES), jnp.float32)
    line = pltpu.VMEM((1, LANES), jnp.float32)
    answer, ahead, residual, applied, step = pl.pallas_call(
        functools.partial(kernel, shape, interp),
        out_shape=(tile, tile, tile, tile, line),
        in_specs=[pl.BlockSpec(memory_space=pl.ANY)] * 8,
        out_specs=(pl.BlockSpec(memory_space=pltpu.VMEM),) * 5,
        scratch_shapes=[
            *[pltpu.VMEM(value.shape, value.dtype) for value in operands],
            pltpu.SemaphoreType.DMA((len(operands),)),
            pltpu.VMEM((own_rows, LANES), jnp.float32),
            pltpu.VMEM((2 * own_rows, LANES), jnp.bfloat16),
            pltpu.VMEM((groups, LANES, 8 * LANES), jnp.bfloat16),
            pltpu.VMEM((2 * ITERS, groups * 8, LANES), jnp.int32),
            pltpu.VMEM((groups * 8, LANES), jnp.int32),
            pltpu.VMEM((con_tiles * 8, LANES), jnp.float32),
            pltpu.VMEM((cell_rows + 8 * con_tiles, LANES), jnp.float32),
            pltpu.VMEM((2 * own_rows, LANES), jnp.float32),
            pltpu.VMEM((LANES, 2 * far_rows), jnp.float32),
            pltpu.VMEM((2 * blocks * block_rows, LANES), jnp.float32),
            exchange,
            landing,
            exchange,
            exchange,
            pltpu.VMEM((ROUNDS, 1, LANES), jnp.float32),
            pltpu.VMEM((ROUNDS, near, 1, LANES), jnp.float32),
            pltpu.VMEM((ROUNDS, 1, LANES), jnp.float32),
            pltpu.VMEM((ROUNDS, far, 1, LANES), jnp.float32),
            pltpu.SemaphoreType.DMA((2,)),
            pltpu.SemaphoreType.DMA((2, 2)),
            pltpu.SemaphoreType.DMA((2,)),
            pltpu.SemaphoreType.DMA((2, 2)),
            pltpu.SemaphoreType.DMA((ROUNDS,)),
            pltpu.SemaphoreType.DMA((ROUNDS,)),
            pltpu.SemaphoreType.DMA((ROUNDS,)),
            pltpu.SemaphoreType.DMA((ROUNDS,)),
        ],
        compiler_params=pltpu.CompilerParams(
            collective_id=0, has_side_effects=True, vmem_limit_bytes=60 * 1024 * 1024
        ),
    )(*operands)
    scale = step[0, 0]
    return (
        (answer + scale * ahead).reshape(own),
        (residual - scale * applied).reshape(own),
    )


def solution(mesh):
    placed = (
        P(("gx", "gy")),
        P(("gx", "gy")),
        P(None, ("gx", "gy")),
        P(("gx", "gy")),
        P(None, ("gx", "gy")),
        P(("gx", "gy")),
        P(None, ("gx", "gy")),
    )
    return jax.shard_map(
        functools.partial(on_device, (mesh.shape["gx"], mesh.shape["gy"])),
        mesh=mesh,
        in_specs=placed,
        out_specs=(P(("gx", "gy")), P(("gx", "gy"))),
        check_vma=False,
    )
```

```python
import functools

import jax
import jax.numpy as jnp
import numpy as np
from jax import lax
from jax.experimental import pallas as pl
from jax.experimental.pallas import tpu as pltpu
from jax.sharding import PartitionSpec as P

ITERS = 3
LANES = 128
SUMS = 4
ROUNDS = 2
UNROLL = 9
MESH = pl.DeviceIdType.MESH


def lagrange(node_list, points):
    node_count = len(node_list)
    values = np.ones((len(points), node_count))
    derivs = np.zeros((len(points), node_count))
    for basis_node in range(node_count):
        for other_node in range(node_count):
            if other_node != basis_node:
                values[:, basis_node] = (
                    values[:, basis_node]
                    * (points - node_list[other_node])
                    / (node_list[basis_node] - node_list[other_node])
                )
        for skipped in range(node_count):
            if skipped != basis_node:
                product_term = np.ones(len(points)) / (node_list[basis_node] - node_list[skipped])
                for other_node in range(node_count):
                    if other_node != basis_node and other_node != skipped:
                        product_term = (
                            product_term
                            * (points - node_list[other_node])
                            / (node_list[basis_node] - node_list[other_node])
                        )
                derivs[:, basis_node] = derivs[:, basis_node] + product_term
    return (values, derivs)


def tables():
    gll_offset = np.sqrt(3.0 / 7.0)
    lobatto = np.array([0.0, (1.0 - gll_offset) / 2.0, 0.5, (1.0 + gll_offset) / 2.0, 1.0])
    inner_point = np.sqrt(5.0 - 2.0 * np.sqrt(10.0 / 7.0)) / 3.0
    outer_point = np.sqrt(5.0 + 2.0 * np.sqrt(10.0 / 7.0)) / 3.0
    inner_weight = (322.0 + 13.0 * np.sqrt(70.0)) / 900.0
    outer_weight = (322.0 - 13.0 * np.sqrt(70.0)) / 900.0
    points = np.array([-outer_point, -inner_point, 0.0, inner_point, outer_point])
    gauss_weights = np.array(
        [outer_weight, inner_weight, 128.0 / 225.0, inner_weight, outer_weight]
    )
    points = (points + 1.0) / 2.0
    gauss_weights = gauss_weights / 2.0
    shapes, slopes = lagrange(lobatto, points)
    fine_points = np.concatenate([lobatto / 2.0, (1.0 + lobatto) / 2.0])
    interp, unused_slopes = lagrange(lobatto, fine_points)
    quad_weights = np.kron(gauss_weights, np.kron(gauss_weights, gauss_weights))
    grad_x = np.kron(slopes, np.kron(shapes, shapes))
    grad_y = np.kron(shapes, np.kron(slopes, shapes))
    grad_z = np.kron(shapes, np.kron(shapes, slopes))
    stiffness = np.zeros((125, 125))
    for gradient in (grad_x, grad_y, grad_z):
        stiffness = stiffness + gradient.T @ (quad_weights[:, None] * gradient)
    return (interp.astype(np.float32), stiffness.astype(np.float32))


def round_up(value, step):
    return -(-value // step) * step


def split(value):
    high = value.astype(jnp.bfloat16)
    low = (value - high.astype(jnp.float32)).astype(jnp.bfloat16)
    return high, low


def kernel(
    shape,
    interp,
    *refs,
):
    inputs, refs = refs[:8], refs[8:]
    answer_ref, ahead_ref, residual_ref, applied_ref, step_ref = refs[:5]
    staged, refs = refs[5:13], refs[13:]
    right_ref, reaction_ref, cells_ref, level_ref, masters_ref, rows_ref, lists_ref, stiff_ref = staged
    (
    load_sem,
    own_values,
    own_table,
    onehot,
    lane_of,
    row_of,
    weights,
    cell_buf,
    own_acc,
    far_acc,
    con_acc,
    out_src,
    out_dst,
    back_src,
    back_dst,
    part,
    first_buf,
    mid_part,
    second_buf,
    out_send,
    out_recv,
    back_send,
    back_recv,
    first_send,
    first_recv,
    second_send,
    second_recv,
    ) = refs
    loads = [
        pltpu.make_async_copy(source, target, load_sem.at[i])
        for i, (source, target) in enumerate(zip(inputs, staged))
    ]
    order = [0, 6, 2, 4, 5, 3, 1, 7]
    for i in order:
        loads[i].start()
    nx, ny = shape
    count = nx * ny
    inner = lax.axis_index("gy")
    me = lax.axis_index("gx") * ny + inner
    upper = lax.div(2 * inner, ny)

    def place(rank):
        return (lax.div(rank, ny), lax.rem(rank, ny))

    blocks, listed = lists_ref.shape
    half = blocks // 2
    own_rows = right_ref.shape[0]
    block_rows = listed // LANES
    ghost_rows = blocks * block_rows
    side_rows = half * block_rows
    con_rows = rows_ref.shape[0]
    con_pad = round_up(con_rows, 8)
    far_rows = ghost_rows + con_pad
    nodes = masters_ref.shape[0]
    points = cells_ref.shape[0]
    cell_rows = round_up(points, 8)
    cell_groups = cell_rows // 8
    list_groups = ghost_rows // 8
    side_groups = list_groups // 2
    per_group = 8 // block_rows
    con_base = cell_groups
    work_groups = cell_groups + con_rows
    list_base = work_groups
    near, far = phases(count)
    near_id, far_id = lax.rem(me, near), lax.div(me, near)
    sent_first = 1 - upper
    slow = min(1, half - 1)
    slow_group = slow // per_group
    group_order = [slow_group] + [q for q in range(side_groups) if q != slow_group]
    block_order = [slow] + [k for k in range(half) if k != slow]

    def offset(side, k):
        return (k + 1) * (1 - 2 * side)

    def near_peer(step):
        return far_id * near + lax.rem(near_id + step, near)

    def far_peer(step):
        return lax.rem(far_id + step, far) * near + near_id

    def ring_peer(distance):
        return lax.rem(me + distance + count, count)

    barrier = pltpu.get_barrier_semaphore()
    peers = []
    if far > 1:
        peers += [ring_peer(offset(side, k)) for side in range(2) for k in range(half)]
    peers += [near_peer(step) for step in range(1, near)]
    peers += [far_peer(step) for step in range(1, far)]
    for peer in peers:
        pl.semaphore_signal(barrier, inc=1, device_id=place(peer), device_id_type=MESH)

    def put(at, slots, shown):
        size = slots.shape[0]
        for copy in range(2 * ITERS):
            lane_of[copy, at : at + size, :] = lax.rem(slots, LANES)
        row_of[at : at + size, :] = jnp.where(shown, lax.div(slots, LANES), -1)

    def held(slots):
        rows = lax.div(slots, LANES) - own_rows
        shown = jnp.full(slots.shape, True)
        for side in range(2):
            for k in range(half):
                other = me - offset(side, k)
                low = (side * half + k) * block_rows
                outside = jnp.logical_or(other < 0, other >= count)
                hidden = jnp.logical_and(rows >= low, rows < low + block_rows)
                shown = jnp.logical_and(shown, jnp.logical_not(jnp.logical_and(hidden, outside)))
        return shown

    lane_iota = lax.broadcasted_iota(jnp.int32, (LANES, LANES), 0)

    def build(g, carry):
        lanes = lane_of[0, pl.ds(pl.multiple_of(g * 8, 8), 8), :]
        for i in range(8):
            hit = jnp.where(lanes[i : i + 1, :] == lane_iota, 1.0, 0.0)
            onehot[g, :, i * LANES : (i + 1) * LANES] = hit.astype(jnp.bfloat16)
        return carry

    iota8 = lax.broadcasted_iota(jnp.int32, (8, LANES), 0)

    once = 1 + lax.div(inner, ny)

    def apart(work):
        def body(i, carry):
            work()
            return carry

        lax.fori_loop(0, once, body, 0)

    def group(g):
        return pl.ds(pl.multiple_of(g * 8, 8), 8)

    def gather(g, table):
        depth = table.shape[0] // 2
        spread = jnp.dot(table[...], onehot[g], preferred_element_type=jnp.float32)
        rows = row_of[group(g), :]
        found = []
        for i in range(8):
            wanted = jnp.broadcast_to(rows[i : i + 1, :], (8, LANES)) - iota8
            high = jnp.zeros((8, LANES), jnp.float32)
            low = high
            for k in range(depth // 8):
                hit = wanted == 8 * k
                at, cols = 8 * k, slice(i * LANES, (i + 1) * LANES)
                high = jnp.where(hit, spread[at : at + 8, cols], high)
                low = jnp.where(hit, spread[depth + at : depth + at + 8, cols], low)
            found.append(jnp.sum(high + low, axis=0, keepdims=True))
        return jnp.concatenate(found, axis=0)

    def pick(lanes, rows, lines, found):
        for k, line in lines:
            moved = jnp.take_along_axis(
                jnp.broadcast_to(line, (8, LANES)), lanes, axis=1, mode="promise_in_bounds"
            )
            found = jnp.where(rows == k, moved, found)
        return found

    def parts_of(values):
        high = values.astype(jnp.bfloat16).astype(jnp.float32)
        return high, values - high

    def against(placed, g, first):
        return lax.dot_general(
            placed,
            onehot[g, :, first * LANES : first * LANES + placed.shape[1]],
            (((1,), (1,)), ((), ())),
            preferred_element_type=jnp.float32,
        )

    def scatter(g, values, base, depth, first=0):
        rows = row_of[group(g), :] - base
        high, low = parts_of(values)
        row_iota = lax.broadcasted_iota(jnp.int32, (depth, LANES), 0)
        columns = []
        for i in range(values.shape[0]):
            hit = rows[first + i : first + i + 1, :] == row_iota
            upper_part = jnp.where(hit, high[i : i + 1, :], 0.0).astype(jnp.bfloat16)
            lower_part = jnp.where(hit, low[i : i + 1, :], 0.0).astype(jnp.bfloat16)
            columns.append(jnp.concatenate([upper_part, lower_part], axis=0))
        return against(jnp.concatenate(columns, axis=1), g, first)

    def scatter_far(g, values):
        rows = row_of[group(g), :] - own_rows
        high, low = parts_of(values)
        row_iota = lax.broadcasted_iota(jnp.int32, (ghost_rows, LANES), 0)
        con_iota = lax.broadcasted_iota(jnp.int32, (2 * con_pad, LANES), 0)
        con_row = ghost_rows + lax.rem(con_iota, con_pad)
        columns = []
        for i in range(8):
            one = rows[i : i + 1, :]
            hit = one == row_iota
            con_hit = one == con_row
            top, bottom = high[i : i + 1, :], low[i : i + 1, :]
            both = jnp.where(con_iota < con_pad, top, bottom)
            columns.append(
                jnp.concatenate(
                    [
                        jnp.where(hit, top, 0.0).astype(jnp.bfloat16),
                        jnp.where(hit, bottom, 0.0).astype(jnp.bfloat16),
                        jnp.where(con_hit, both, 0.0).astype(jnp.bfloat16),
                    ],
                    axis=0,
                )
            )
        placed = jnp.concatenate(columns, axis=1)
        return lax.dot_general(
            onehot[g], placed, (((1,), (1,)), ((), ())), preferred_element_type=jnp.float32
        )

    def folded(both):
        depth = both.shape[0] // 2
        return both[0:depth] + both[depth : 2 * depth]

    def store(table, value):
        high, low = split(value)
        size = value.shape[0]
        table[0:size, :] = high
        table[size : 2 * size, :] = low

    def out_copy(turn, side, k):
        j = side * half + k
        return pltpu.make_async_remote_copy(
            src_ref=out_src.at[turn, j],
            dst_ref=out_dst.at[turn, j],
            send_sem=out_send.at[side],
            recv_sem=out_recv.at[side, int(k == slow)],
            device_id=place(ring_peer(offset(side, k))),
            device_id_type=MESH,
        )

    def back_copy(turn, side, k):
        j = side * half + k
        return pltpu.make_async_remote_copy(
            src_ref=back_src.at[turn, j],
            dst_ref=back_dst.at[turn, j],
            send_sem=back_send.at[side],
            recv_sem=back_recv.at[side, int(k == slow)],
            device_id=place(ring_peer(-offset(side, k))),
            device_id_type=MESH,
        )

    def near_copy(turn, step):
        return pltpu.make_async_remote_copy(
            src_ref=part.at[turn],
            dst_ref=first_buf.at[turn, near_id],
            send_sem=first_send.at[turn],
            recv_sem=first_recv.at[turn],
            device_id=place(near_peer(step)),
            device_id_type=MESH,
        )

    def far_copy(turn, step):
        return pltpu.make_async_remote_copy(
            src_ref=mid_part.at[turn],
            dst_ref=second_buf.at[turn, far_id],
            send_sem=second_send.at[turn],
            recv_sem=second_recv.at[turn],
            device_id=place(far_peer(step)),
            device_id_type=MESH,
        )

    out_ends = (out_src, out_dst, out_send, out_recv)
    back_ends = (back_src, back_dst, back_send, back_recv)

    def list_values(turn, side, q):
        lines = [(r, own_values[r : r + 1, :]) for r in range(own_rows)]
        at = group(list_base + side * side_groups + q)
        zero = jnp.zeros((8, LANES), jnp.float32)
        found = pick(lane_of[2 * turn, at, :], row_of[at, :], lines, zero)
        for r in range(per_group):
            j = side * half + q * per_group + r
            out_src[turn, j] = found[r * block_rows : (r + 1) * block_rows]

    def arrived(turn, side, mixed, which):
        source = turn
        if mixed is not None:
            source = ITERS
            for k in which:
                j = side * half + k
                out_dst[source, j] = mixed(*[out_dst[t, j] for t in range(turn + 1)])
        return [
            (k * block_rows + r, out_dst[source, side * half + k, r : r + 1, :])
            for k in which
            for r in range(block_rows)
        ]

    def settle(ref, sem):
        pltpu.make_async_copy(ref, ref, sem).wait()

    def take_most(ends, turn, side):
        if half > 1:
            settle(ends[1].at[turn, pl.ds(side * half, half - 1)], ends[3].at[side, 0])

    def take_slow(ends, turn, side):
        settle(ends[1].at[turn, pl.ds(side * half, 1)], ends[3].at[side, 1])

    def sent(ends, turn, side):
        settle(ends[0].at[turn, pl.ds(side * half, half)], ends[2].at[side])

    def begin_apply(turn, vector):
        own_values[...] = vector
        for side in (sent_first, upper):
            for q in group_order:
                list_values(turn, side, q)
                if turn == 0 and side is sent_first and q == slow_group:
                    pl.semaphore_wait(barrier, len(peers))
                for k in block_order:
                    if k // per_group == q:
                        out_copy(turn, side, k).start()

    def apply(turn, vector, mixed, begin, middle, ready=lambda: None):
        store(own_table, vector)

        def take_own(g, carry):
            cell_buf[group(g), :] = gather(g, own_table)
            return carry

        lax.fori_loop(0, work_groups, take_own, 0, unroll=UNROLL)

        early, late = sent_first, upper
        take_most(out_ends, turn, early)
        take_slow(out_ends, turn, early)
        lines = arrived(turn, early, mixed, range(half))
        base = own_rows + early * side_rows
        for g in range(work_groups):
            at = slice(8 * g, 8 * g + 8)
            cell_buf[at, :] = pick(lane_of[2 * turn, at, :], row_of[at, :] - base, lines, cell_buf[at, :])

        base = own_rows + late * side_rows
        if half > 1:
            take_most(out_ends, turn, late)
            lines = arrived(turn, late, mixed, block_order[1:])
            for g in range(work_groups):
                at = slice(8 * g, 8 * g + 8)
                cell_buf[at, :] = pick(lane_of[2 * turn + 1, at, :], row_of[at, :] - base, lines, cell_buf[at, :])

        take_slow(out_ends, turn, late)
        lines = arrived(turn, late, mixed, [slow])
        resolved = []
        for h in range(con_rows):
            at, to = slice(8 * (con_base + h), 8 * (con_base + h) + 8), slice(8 * h, 8 * h + 8)
            found = pick(lane_of[2 * turn + 1, at, :], row_of[at, :] - base, lines, cell_buf[at, :])
            resolved.append((h, jnp.sum(weights[to, :] * found, axis=0, keepdims=True)))
        found = []
        ahead = min(4, cell_groups)
        for g in range(cell_groups):
            at = slice(8 * g, 8 * g + 8)
            lanes, rows = lane_of[2 * turn + 1, at, :], row_of[at, :]
            found.append(pick(lanes, rows - base, lines, cell_buf[at, :]))
            if g >= ahead:
                found[g] = pick(lanes, rows - (own_rows + ghost_rows), resolved, found[g])
        for g in range(ahead):
            at = slice(8 * g, 8 * g + 8)
            lanes, rows = lane_of[2 * turn + 1, at, :], row_of[at, :]
            found[g] = pick(lanes, rows - (own_rows + ghost_rows), resolved, found[g])
        nodal = jnp.concatenate(found, axis=0)
        contrib = scale * jnp.dot(
            stiff_ref[...],
            nodal,
            precision=lax.Precision.HIGHEST,
            preferred_element_type=jnp.float32,
        )
        cell_buf[0:cell_rows, :] = contrib
        weighted = reaction_ref[...] * vector
        energy = jnp.sum(nodal * contrib, axis=0, keepdims=True)
        energy = energy + jnp.sum(weighted * vector, axis=0, keepdims=True)
        begin(energy)


        def give_all_far():
            total = jnp.zeros((LANES, 2 * far_rows), jnp.float32)
            for g in range(cell_groups):
                total = total + scatter_far(g, cell_buf[8 * g : 8 * g + 8, :])
            far_acc[...] = total

        apart(give_all_far)
        total = jnp.transpose(far_acc[...])
        spread = total[0:ghost_rows] + total[ghost_rows : 2 * ghost_rows]
        summed = folded(total[2 * ghost_rows : 2 * far_rows])
        for h in range(con_rows):
            shares = weights[8 * h : 8 * h + 8, :] * summed[h : h + 1]
            cell_buf[8 * (con_base + h) : 8 * (con_base + h) + 8, :] = shares

        def give_con():
            total = jnp.zeros((2 * ghost_rows, LANES), jnp.float32)
            for h in range(con_rows):
                values = cell_buf[8 * (con_base + h) : 8 * (con_base + h) + nodes, :]
                total = total + scatter(con_base + h, values, own_rows, ghost_rows)
            con_acc[...] = total

        apart(give_con)
        spread = spread + folded(con_acc[...])
        for j in range(blocks):
            back_src[turn, j] = spread[j * block_rows : (j + 1) * block_rows]
        for side in (late, early):
            for k in block_order:
                back_copy(turn, side, k).start()
        middle()
        own_acc[...] = jnp.zeros_like(own_acc)

        def give_own(g, carry):
            own_acc[...] += scatter(g, cell_buf[group(g), :], 0, own_rows)
            return carry

        lax.fori_loop(0, work_groups, give_own, 0, unroll=UNROLL)
        def give_lists(side, which):
            def work():
                both = own_acc[...]
                for q in range(side_groups):
                    chosen = [k for k in which if k // per_group == q]
                    if not chosen:
                        continue
                    values = jnp.concatenate([back_dst[turn, side * half + k] for k in chosen], axis=0)
                    first = (chosen[0] - q * per_group) * block_rows
                    both = both + scatter(list_base + side * side_groups + q, values, 0, own_rows, first)
                own_acc[...] = both

            apart(work)

        sent(out_ends, turn, early)
        sent(out_ends, turn, late)
        take_most(back_ends, turn, late)
        take_slow(back_ends, turn, late)
        give_lists(late, range(half))
        take_most(back_ends, turn, early)
        if half > 1:
            give_lists(early, sorted(block_order[1:]))
        ready()
        take_slow(back_ends, turn, early)
        give_lists(early, [slow])
        sent(back_ends, turn, late)
        sent(back_ends, turn, early)
        both = own_acc[...]
        return folded(both) + weighted

    def dot(one, two):
        return jnp.sum(one * two, axis=0, keepdims=True)

    lane = lax.broadcasted_iota(jnp.int32, (1, LANES), 1)
    width = LANES // SUMS

    def sums_start(turn, parts):
        total = jnp.sum(jnp.concatenate(parts, axis=0), axis=1, keepdims=True)
        mine = jnp.zeros((1, LANES), jnp.float32)
        for k in range(len(parts)):
            mine = jnp.where(lax.div(lane, width) == k, total[k : k + 1], mine)
        part[turn] = mine
        first_buf[turn, near_id] = mine

    def sums_send(turn):
        for step in range(1, near):
            near_copy(turn, step).start()

    def near_total(turn):
        others = pl.ds(0, near - 1)
        settle(first_buf.at[turn, others], first_send.at[turn])
        settle(first_buf.at[turn, others], first_recv.at[turn])
        mine = first_buf[turn, 0]
        for k in range(1, near):
            mine = mine + first_buf[turn, k]
        return mine

    def sums_middle(turn):
        sums_send(turn)
        if far == 1:
            return
        mine = near_total(turn)
        mid_part[turn] = mine
        second_buf[turn, far_id] = mine
        for step in range(1, far):
            far_copy(turn, step).start()

    def sums_end(turn):
        if far == 1:
            total = near_total(turn)
        else:
            others = pl.ds(0, far - 1)
            settle(second_buf.at[turn, others], second_send.at[turn])
            settle(second_buf.at[turn, others], second_recv.at[turn])
            total = second_buf[turn, 0]
            for k in range(1, far):
                total = total + second_buf[turn, k]
        return [total[:, k * width : k * width + 1] for k in range(SUMS)]

    loads[0].wait()
    loads[6].wait()
    for side in range(2):
        for k in range(half):
            j = side * half + k
            other = me + offset(side, k)
            inside = jnp.logical_and(other >= 0, other < count)
            for q in range(block_rows):
                at = list_base * 8 + j * block_rows + q
                put(at, lists_ref[j : j + 1, q * LANES : (q + 1) * LANES], inside)
    start = right_ref[...]
    begin_apply(0, start)
    for i in order[2:]:
        loads[i].wait()
    for copy in range(2 * ITERS):
        lane_of[copy, points:cell_rows, :] = jnp.zeros((cell_rows - points, LANES), jnp.int32)
    row_of[points:cell_rows, :] = jnp.full((cell_rows - points, LANES), -1, jnp.int32)
    slots = cells_ref[...]
    put(0, slots, held(slots))
    weights[...] = jnp.zeros_like(weights)
    for h in range(con_rows):
        at = (con_base + h) * 8
        for copy in range(2 * ITERS):
            lane_of[copy, at : at + 8, :] = jnp.zeros((8, LANES), jnp.int32)
        row_of[at : at + 8, :] = jnp.full((8, LANES), -1, jnp.int32)
        slots = masters_ref[:, h * LANES : (h + 1) * LANES]
        put(at, slots, held(slots))
        chosen = rows_ref[h : h + 1, :]
        for k in range(nodes):
            weight = jnp.zeros((1, LANES), jnp.float32)
            for t in range(interp.shape[0]):
                weight = jnp.where(chosen == t, float(interp[t, k]), weight)
            weights[h * 8 + k : h * 8 + k + 1, :] = weight
    lax.fori_loop(0, onehot.shape[0], build, 0)
    scale = jnp.exp2(-level_ref[...].astype(jnp.float32))

    first = apply(0, start, None, lambda energy: None, lambda: None)
    begin_apply(1, first)
    known = [dot(start, start), dot(start, first), dot(first, first)]
    second = apply(
        1,
        first,
        None,
        lambda energy: sums_start(0, known + [energy]),
        lambda: sums_middle(0),
    )
    begin_apply(2, second)
    m0, m1, m2, m3 = sums_end(0)
    step0 = m0 / m1
    norm1 = m0 - 2.0 * step0 * m1 + step0 * step0 * m2
    product1 = m1 - 2.0 * step0 * m2 + step0 * step0 * m3
    ratio1 = norm1 / m0
    step1 = norm1 / (product1 - ratio1 * norm1 / step0)

    def next_residual(zeroth, once, twice):
        before = zeroth - step0 * once
        along = once - step0 * twice + ratio1 * once
        return before, along, before - step1 * along

    before, applied_dir, residual = next_residual(start, first, second)
    direction = before + ratio1 * start
    answer = step0 * start + step1 * direction
    square = dot(residual, residual)
    scalars = []

    def last_sums():
        norm2, product2, unused_a, unused_b = sums_end(1)
        ratio2 = norm2 / norm1
        scalars.extend([ratio2, norm2 / (product2 - ratio2 * norm2 / step1)])

    applied = apply(
        2,
        residual,
        lambda *held: next_residual(*held)[2],
        lambda energy: sums_start(1, [square, energy]),
        lambda: sums_middle(1),
        last_sums,
    )
    ratio2, step2 = scalars
    answer_ref[...] = answer
    ahead_ref[...] = residual + ratio2 * direction
    residual_ref[...] = residual
    applied_ref[...] = applied + ratio2 * applied_dir
    step_ref[...] = jnp.broadcast_to(step2, step_ref.shape)


def phases(count):
    if count <= 64:
        return count, 1
    near = 1
    while near * near < count:
        near *= 2
    return near, count // near


def on_device(shape, right_side, reaction, cell_slots, cell_level, con_masters, con_rows, send_lists):
    interp, stiffness = tables()
    own = right_side.shape[0]
    own_rows = own // LANES
    blocks, listed = send_lists.shape
    block_rows = listed // LANES
    con_tiles = con_rows.shape[0] // LANES
    points = cell_slots.shape[0]
    cell_rows = round_up(points, 8)
    far_rows = blocks * block_rows + round_up(con_tiles, 8)
    groups = cell_rows // 8 + blocks * block_rows // 8 + con_tiles
    padded = np.zeros((cell_rows, cell_rows), np.float32)
    padded[:points, :points] = stiffness
    count = shape[0] * shape[1]
    near, far = phases(count)
    operands = [
        right_side.reshape(own_rows, LANES),
        reaction.reshape(own_rows, LANES),
        cell_slots,
        cell_level.reshape(1, -1),
        con_masters,
        con_rows.reshape(con_tiles, LANES),
        send_lists,
        jnp.asarray(padded),
    ]
    exchange = pltpu.VMEM((ITERS, blocks, block_rows, LANES), jnp.float32)
    landing = pltpu.VMEM((ITERS + 1, blocks, block_rows, LANES), jnp.float32)
    tile = pltpu.VMEM((own_rows, LANES), jnp.float32)
    line = pltpu.VMEM((1, LANES), jnp.float32)
    answer, ahead, residual, applied, step = pl.pallas_call(
        functools.partial(kernel, shape, interp),
        out_shape=(tile, tile, tile, tile, line),
        in_specs=[pl.BlockSpec(memory_space=pl.ANY)] * 8,
        out_specs=(pl.BlockSpec(memory_space=pltpu.VMEM),) * 5,
        scratch_shapes=[
            *[pltpu.VMEM(value.shape, value.dtype) for value in operands],
            pltpu.SemaphoreType.DMA((len(operands),)),
            pltpu.VMEM((own_rows, LANES), jnp.float32),
            pltpu.VMEM((2 * own_rows, LANES), jnp.bfloat16),
            pltpu.VMEM((groups, LANES, 8 * LANES), jnp.bfloat16),
            pltpu.VMEM((2 * ITERS, groups * 8, LANES), jnp.int32),
            pltpu.VMEM((groups * 8, LANES), jnp.int32),
            pltpu.VMEM((con_tiles * 8, LANES), jnp.float32),
            pltpu.VMEM((cell_rows + 8 * con_tiles, LANES), jnp.float32),
            pltpu.VMEM((2 * own_rows, LANES), jnp.float32),
            pltpu.VMEM((LANES, 2 * far_rows), jnp.float32),
            pltpu.VMEM((2 * blocks * block_rows, LANES), jnp.float32),
            exchange,
            landing,
            exchange,
            exchange,
            pltpu.VMEM((ROUNDS, 1, LANES), jnp.float32),
            pltpu.VMEM((ROUNDS, near, 1, LANES), jnp.float32),
            pltpu.VMEM((ROUNDS, 1, LANES), jnp.float32),
            pltpu.VMEM((ROUNDS, far, 1, LANES), jnp.float32),
            pltpu.SemaphoreType.DMA((2,)),
            pltpu.SemaphoreType.DMA((2, 2)),
            pltpu.SemaphoreType.DMA((2,)),
            pltpu.SemaphoreType.DMA((2, 2)),
            pltpu.SemaphoreType.DMA((ROUNDS,)),
            pltpu.SemaphoreType.DMA((ROUNDS,)),
            pltpu.SemaphoreType.DMA((ROUNDS if far > 1 else 1,)),
            pltpu.SemaphoreType.DMA((ROUNDS if far > 1 else 1,)),
        ],
        compiler_params=pltpu.CompilerParams(
            collective_id=0, has_side_effects=True, vmem_limit_bytes=60 * 1024 * 1024
        ),
    )(*operands)
    scale = step[0, 0]
    return (
        (answer + scale * ahead).reshape(own),
        (residual - scale * applied).reshape(own),
    )


def solution(mesh):
    placed = (
        P(("gx", "gy")),
        P(("gx", "gy")),
        P(None, ("gx", "gy")),
        P(("gx", "gy")),
        P(None, ("gx", "gy")),
        P(("gx", "gy")),
        P(None, ("gx", "gy")),
    )
    return jax.shard_map(
        functools.partial(on_device, (mesh.shape["gx"], mesh.shape["gy"])),
        mesh=mesh,
        in_specs=placed,
        out_specs=(P(("gx", "gy")), P(("gx", "gy"))),
        check_vma=False,
    )
```
